32 devices in a mesh: dp: 4 (over y, x), mp: 8 (over z, core).
Axes of the slice: x: 2, y: 2, z: 4, core: 2. Of those that a mesh axis runs over, the one named last changes fastest.
Arguments:
- image: bfloat16 [4, 2048, 1280], P('dp', 'mp'), may hold values from -6 to 6
- ln_gain: float32 [1280], replicated, may hold values from 0.1 to 1.9
- fc1_weight: bfloat16 [1280, 5120], P(None, ('dp', 'mp')), may hold values from -0.15625 to 0.15625
- fc2_weight: bfloat16 [5120, 1280], P(('dp', 'mp')), may hold values from -0.078125 to 0.078125
- projector_weight: bfloat16 [1280, 8192], P(None, 'mp'), may hold values from -0.15625 to 0.15625
- kv_weight: bfloat16 [8192, 8, 2, 128], P('mp'), may hold values from -0.0625 to 0.0625
- text: bfloat16 [4, 128, 8192], P('dp'), may hold values from -480 to 480
- q_weight: bfloat16 [8192, 8192], P(None, 'mp'), may hold values from -0.0625 to 0.0625
- o_weight: bfloat16 [8192, 8192], P('mp'), may hold values from -0.0625 to 0.0625
- tile_count: int32 [4], P('dp'), may hold values from 1 to 4
- text_start: int32 [4], P('dp'), may hold values from 0 to 63
Outputs:
- attended: bfloat16 [4, 128, 8192], P('dp', 'mp')
The draws below stay inside these ranges and needn't reach their ends.
All inputs are finite; a program needn't handle non-finite values.
Results may differ from the reference program's by a relative error of at most 0.035.
Values may be sent and summed in bfloat16 or wider, within the bound.
A program may use at most 128 MiB of HBM per device.

```python
import jax
import jax.numpy as jnp
from jax import lax

D_VIS = 1280
VIS_FF = 5120
HEADS = 64
KV_HEADS = 8
HEAD_DIM = 128
D = 8192
MAX_TILES = 4
TILE_TOK = 512
TEXT = 128
IMG = 2048
SAMPLES = 4


def draw_text(key, part):
    base = jax.random.normal(key, (SAMPLES, TEXT, D), jnp.float32)
    return jnp.clip(base, -6.0, 6.0).astype(jnp.bfloat16)


def touch_ends(entries, stream_key, low, top_value):
    longest = entries.shape.index(max(entries.shape))
    spots = []
    for shift in (0, 1):
        where = [jax.random.randint(jax.random.fold_in(stream_key, axis), (), 0, length) for axis, length in enumerate(entries.shape)]
        where[longest] = (where[longest] + shift) % entries.shape[longest]
        spots.append(tuple(where))
    return entries.at[spots[0]].set(low).at[spots[1]].set(top_value)


def block_levels(rng, extent, shards, least, largest):
    def one(dim, blocks):
        draws = jax.random.uniform(jax.random.fold_in(jax.random.fold_in(rng, 6), dim), (blocks,), jnp.float32, least / len(shards), largest / len(shards))
        return jnp.repeat(jnp.exp(draws), extent[dim] // blocks).reshape((-1,) + (1,) * (len(extent) - dim - 1))

    level = one(*shards[0])
    for cut in shards[1:]:
        level = level * one(*cut)
    return level


def centred(stream_key, shape, scale, reach, shards=(), held_as=jnp.bfloat16):
    result = jax.random.normal(stream_key, shape, jnp.float32) * scale
    if len(shards) > 0:
        result = block_levels(stream_key, shape, shards, -0.22, 0.18) * result
    return jnp.clip(result, min=-reach, max=reach).astype(held_as)


def setup_inputs(seed: int = 0) -> dict:
    splits = jax.random.split(jax.random.key(seed), 12)
    return {
        "image": centred(splits[0], (SAMPLES, IMG, D_VIS), 1.0, 6.0, ((0, 4), (1, 8))),
        "ln_gain": jnp.clip(1.0 + 0.18 * jax.random.normal(splits[1], (D_VIS,), jnp.float32), 0.1, 1.9),
        "fc1_weight": centred(splits[2], (D_VIS, VIS_FF), D_VIS ** -0.5, 0.15625, ((1, 32),)),
        "fc2_weight": centred(splits[3], (VIS_FF, D_VIS), VIS_FF ** -0.5, 0.078125, ((0, 32),)),
        "projector_weight": centred(splits[4], (D_VIS, D), D_VIS ** -0.5, 0.15625, ((1, 8),)),
        "kv_weight": centred(splits[5], (D, KV_HEADS, 2, HEAD_DIM), D ** -0.5, 0.0625, ((0, 8),)),
        "text": draw_text(jax.random.fold_in(splits[11], 71), 0),
        "q_weight": centred(splits[7], (D, D), D ** -0.5, 0.0625, ((1, 8),)),
        "o_weight": centred(splits[8], (D, D), D ** -0.5, 0.0625, ((0, 8),)),
        "tile_count": touch_ends(jax.random.randint(splits[9], (SAMPLES,), 1, MAX_TILES + 1), jax.random.fold_in(splits[9], 1), 1, MAX_TILES).astype(jnp.int32),
        "text_start": touch_ends(jax.random.randint(splits[10], (SAMPLES,), 0, TEXT // 2), jax.random.fold_in(splits[10], 1), 0, (TEXT // 2) - 1).astype(jnp.int32),
    }


def layer_norm(values, gain):
    center = values - lax.optimization_barrier(jnp.mean(values, axis=-1, keepdims=True))
    spread = lax.optimization_barrier(jnp.mean(center * center, axis=-1, keepdims=True))
    return center * lax.rsqrt(spread + 1e-05) * gain

def reference(image, ln_gain, fc1_weight, fc2_weight, projector_weight, kv_weight, text, q_weight, o_weight, tile_count, text_start):
    group_size = HEADS // KV_HEADS
    scale = 1.0 / HEAD_DIM ** 0.5
    outputs = []
    for sample in range(SAMPLES):
        inputs = image[sample].astype(jnp.float32)
        normed = layer_norm(inputs, ln_gain).astype(jnp.bfloat16)
        hidden = jax.nn.gelu(jnp.dot(normed, fc1_weight, preferred_element_type=jnp.float32), approximate=False).astype(jnp.bfloat16)
        encoded = (inputs + jnp.dot(hidden, fc2_weight, preferred_element_type=jnp.float32)).astype(jnp.bfloat16)
        features = jnp.dot(encoded, projector_weight, preferred_element_type=jnp.float32).astype(jnp.bfloat16)
        projected = jnp.dot(features, kv_weight.reshape(D, KV_HEADS * 2 * HEAD_DIM), preferred_element_type=jnp.float32)
        projected = projected.reshape(IMG, KV_HEADS, 2, HEAD_DIM)
        keys = projected[:, :, 0, :]
        keys = keys * lax.rsqrt(lax.optimization_barrier(jnp.mean(keys * keys, axis=-1, keepdims=True)) + 1e-06)
        keys = keys.astype(jnp.bfloat16)
        values = projected[:, :, 1, :].astype(jnp.bfloat16)
        queries = jnp.dot(text[sample], q_weight, preferred_element_type=jnp.float32).astype(jnp.bfloat16)
        queries = queries.reshape(TEXT, KV_HEADS, group_size, HEAD_DIM).transpose(1, 0, 2, 3)
        tiles = jnp.arange(IMG, dtype=jnp.int32) // TILE_TOK
        valid = tiles < tile_count[sample]

        def one_group(operands):
            group_queries, group_keys, group_values = operands
            scores = jnp.einsum('tgd,kd->gtk', group_queries.astype(jnp.float32), group_keys.astype(jnp.float32)) * scale
            scores = jnp.where(valid[None, None, :], scores, -1e+30)
            top = lax.optimization_barrier(jnp.max(scores, axis=-1, keepdims=True))
            weights = jnp.exp(scores - top)
            probs = (weights / lax.optimization_barrier(jnp.sum(weights, axis=-1, keepdims=True))).astype(jnp.bfloat16)
            return jnp.einsum('gtk,kd->tgd', probs.astype(jnp.float32), group_values.astype(jnp.float32))
        attended_heads = lax.map(one_group, (queries, keys.transpose(1, 0, 2), values.transpose(1, 0, 2)))
        attended_heads = attended_heads.transpose(1, 0, 2, 3).reshape(TEXT, HEADS * HEAD_DIM)
        row_mask = (jnp.arange(TEXT, dtype=jnp.int32) >= text_start[sample]).astype(jnp.float32)
        heads_out = (attended_heads * row_mask[:, None]).astype(jnp.bfloat16)
        outputs.append(jnp.dot(heads_out, o_weight, preferred_element_type=jnp.float32).astype(jnp.bfloat16))
    return jnp.stack(outputs, axis=0)
```

```python
import functools

import jax
import jax.numpy as jnp
from jax import lax
from jax.experimental import pallas as pl
from jax.experimental.pallas import tpu as pltpu
from jax.sharding import PartitionSpec as P

HEAD_DIM = 128
TILE_TOK = 512

MESH = pl.DeviceIdType.MESH
CORES = 2


def count_copies(kind):
    name, axis = kind
    size = lax.axis_size(axis)
    if name == "chain":
        return 2 * (size // CORES - 1) + size // CORES
    if name == "partner":
        return size // CORES
    if name == "stride":
        return size // CORES - 1
    return size - 1


def exchange_kernel(kinds, *refs):
    count = len(kinds)
    sources, results = refs[:count], refs[count : 2 * count]
    local_sem = refs[2 * count]
    sends, recvs = refs[2 * count + 1 : 3 * count + 1], refs[3 * count + 1 :]
    axes = sorted({axis for _, axis in kinds})

    barrier = pltpu.get_barrier_semaphore()
    greeted = 0
    for axis in axes:
        size, me = lax.axis_size(axis), lax.axis_index(axis)
        for step in range(1, size):
            pl.semaphore_signal(
                barrier, inc=1, device_id={axis: lax.rem(me + step, size)}, device_id_type=MESH
            )
        greeted += size - 1
    pl.semaphore_wait(barrier, greeted)

    def remote(op, source, result, slot, axis, peer):
        return pltpu.make_async_remote_copy(
            src_ref=source,
            dst_ref=result,
            send_sem=sends[op].at[slot],
            recv_sem=recvs[op].at[slot],
            device_id={axis: peer},
            device_id_type=MESH,
        )

    simple, chains, locals_ = [], [], []
    for op, (name, axis) in enumerate(kinds):
        size, me = lax.axis_size(axis), lax.axis_index(axis)
        source, result = sources[op], results[op]
        core = lax.rem(me, CORES)
        spot = lax.div(me, CORES)
        partner = me + 1 - 2 * core
        if name == "gather":
            for step in range(1, size):
                copy = remote(op, source, result.at[me], step - 1, axis, lax.rem(me + step, size))
                copy.start()
                simple.append(copy)
            locals_.append(pltpu.make_async_copy(source, result.at[me], local_sem.at[op]))
        elif name == "columns":
            width = result.shape[-1]

            def column(index):
                return source.at[:, pl.ds(pl.multiple_of(index * width, width), width)]

            for step in range(1, size):
                peer = lax.rem(me + step, size)
                copy = remote(op, column(peer), result.at[me], step - 1, axis, peer)
                copy.start()
                simple.append(copy)
            locals_.append(pltpu.make_async_copy(column(me), result.at[me], local_sem.at[op]))
        elif name == "scatter":
            for step in range(1, size):
                peer = lax.rem(me + step, size)
                copy = remote(op, source.at[peer], result.at[me], step - 1, axis, peer)
                copy.start()
                simple.append(copy)
            locals_.append(pltpu.make_async_copy(source.at[me], result.at[me], local_sem.at[op]))
        elif name == "partner":
            for chip in range(size // CORES):
                copy = remote(
                    op, source.at[chip * CORES + 1 - core], result.at[chip], chip, axis, partner
                )
                copy.start()
                simple.append(copy)
        elif name == "stride":
            chips = size // CORES
            for step in range(1, chips):
                other = lax.rem(spot + step, chips)
                copy = remote(
                    op, source.at[other], result.at[spot], step - 1, axis, other * CORES + core
                )
                copy.start()
                simple.append(copy)
            locals_.append(pltpu.make_async_copy(source.at[spot], result.at[spot], local_sem.at[op]))
        else:
            chains.append((op, axis, size // CORES, me, core, spot, partner, source, result))
    for copy in locals_:
        copy.start()

    def hop(chain, source, block, slot, peer):
        op, axis, result = chain[0], chain[1], chain[-1]
        return remote(op, source, result.at[block], slot, axis, peer)

    for chain in chains:
        op, axis, chips, me, core, spot, partner, source, result = chain

        @pl.when(spot + 1 < chips)
        def _():
            hop(chain, source, me, 0, me + CORES).start()

        @pl.when(spot > 0)
        def _():
            hop(chain, source, me, chips - 1, me - CORES).start()

    for chain in chains:
        op, axis, chips, me, core, spot, partner, source, result = chain
        hop(chain, source, me, 2 * (chips - 1), partner).start()
        pltpu.make_async_copy(source, result.at[me], local_sem.at[op]).start()
    for step in range(1, max([chain[2] for chain in chains], default=0)):
        for chain in chains:
            op, axis, chips, me, core, spot, partner, source, result = chain
            for sign, base in ((1, 0), (-1, chips - 1)):
                origin_spot = spot - sign * step
                here = (origin_spot >= 0) & (origin_spot < chips)
                onward = (spot + sign >= 0) & (spot + sign < chips)
                block = me - sign * step * CORES

                @pl.when(here)
                def _():
                    held = result.at[block]
                    hop(chain, held, block, base + step - 1, me).wait_recv()

                    @pl.when(onward)
                    def _():
                        hop(chain, held, block, base + step, me + sign * CORES).start()

                    slot = 2 * (chips - 1) + lax.rem(origin_spot - spot + chips, chips)
                    hop(chain, held, block, slot, partner).start()

    for chain in chains:
        op, axis, chips, me, core, spot, partner, source, result = chain
        for step in range(chips):
            for_spot = lax.rem(spot + step, chips)
            block = for_spot * CORES + core
            theirs = for_spot * CORES + 1 - core
            slot = 2 * (chips - 1) + step
            hop(chain, result.at[block], block, slot, partner).wait_send()
            hop(chain, result.at[theirs], theirs, slot, partner).wait_recv()
        for step in range(chips - 1):
            for sign, base in ((1, 0), (-1, chips - 1)):
                origin_spot = spot - sign * step
                sent = (
                    (origin_spot >= 0)
                    & (origin_spot < chips)
                    & (spot + sign >= 0)
                    & (spot + sign < chips)
                )
                block = me - sign * step * CORES

                @pl.when(sent)
                def _():
                    hop(chain, source, block, base + step, partner).wait_send()

        pltpu.make_async_copy(source, result.at[me], local_sem.at[op]).wait()
    for copy in simple:
        copy.wait()
    for copy in locals_:
        copy.wait()


def exchange(kinds, arrays, number):
    kinds = tuple(kinds)
    shapes = []
    for (name, axis), array in zip(kinds, arrays):
        size = lax.axis_size(axis)
        if name in ("gather", "chain"):
            shape = (size,) + array.shape
        elif name == "columns":
            shape = (size, array.shape[0], array.shape[1] // size)
        elif name == "scatter":
            shape = array.shape
        else:
            shape = (size // CORES,) + array.shape[1:]
        shapes.append(jax.ShapeDtypeStruct(shape, array.dtype))
    sems = [pltpu.SemaphoreType.DMA((count_copies(kind),)) for kind in kinds]
    return pl.pallas_call(
        functools.partial(exchange_kernel, kinds),
        out_shape=shapes,
        in_specs=[pl.BlockSpec(memory_space=pl.ANY)] * len(kinds),
        out_specs=[pl.BlockSpec(memory_space=pl.ANY)] * len(kinds),
        scratch_shapes=[pltpu.SemaphoreType.DMA((len(kinds),))] + sems + sems,
        compiler_params=pltpu.CompilerParams(collective_id=number, has_side_effects=True),
        name="exchange",
    )(*arrays)


def swapped(block, axis, bit):
    count = lax.axis_size(axis)
    route = []
    for low in range(count):
        high = low | 1 << bit
        if high != low and high < count:
            route += [(low, high), (high, low)]
    return lax.ppermute(block, axis, route)


def layer_norm(values, gain):
    center = values - jnp.mean(values, axis=-1, keepdims=True)
    spread = jnp.mean(center * center, axis=-1, keepdims=True)
    return center * lax.rsqrt(spread + 1e-05) * gain


def attend_block(block_queries, keys, values, valid, scale, layout):
    scores = (
        jnp.einsum(
            "thd," + layout + "->htk", block_queries, keys, preferred_element_type=jnp.float32
        )
        * scale
    )
    scores = jnp.where(valid[None, None, :], scores, -1e30)
    top = jnp.max(scores, axis=-1, keepdims=True)
    weights = jnp.exp(scores - top)
    probs = (weights / jnp.sum(weights, axis=-1, keepdims=True)).astype(jnp.bfloat16)
    return jnp.einsum("htk," + layout + "->thd", probs, values, preferred_element_type=jnp.float32)


def local(
    image,
    ln_gain,
    fc1_weight,
    fc2_weight,
    projector_weight,
    kv_weight,
    text,
    q_weight,
    o_weight,
    tile_count,
    text_start,
):
    inputs = image[0].astype(jnp.float32)
    group_count = lax.axis_size("mp")
    normed = layer_norm(inputs, ln_gain).astype(jnp.bfloat16)
    up, down, all_normed = exchange(
        (("chain", "mp"), ("chain", "mp"), ("gather", "dp")), (fc1_weight.T, fc2_weight, normed), 0
    )
    up = up.reshape(-1, up.shape[-1])
    down = down.reshape(-1, down.shape[-1])
    all_normed = all_normed.reshape(-1, all_normed.shape[-1])
    hidden = jax.nn.gelu(
        lax.dot_general(
            all_normed, up, (((1,), (1,)), ((), ())), preferred_element_type=jnp.float32
        ),
        approximate=False,
    ).astype(jnp.bfloat16)
    branch = jnp.dot(hidden, down, preferred_element_type=jnp.float32).astype(jnp.bfloat16)
    branch = branch.reshape((lax.axis_size("dp"),) + inputs.shape)

    kv_count = kv_weight.shape[1]
    devices_per_kv = group_count // kv_count
    kv_columns = kv_count * 2 * HEAD_DIM
    flat_kv = kv_weight.reshape(kv_weight.shape[0], kv_columns)
    row_count = projector_weight.shape[0] // lax.axis_size("dp")
    rows = lax.dynamic_slice_in_dim(
        projector_weight, lax.axis_index("dp") * row_count, row_count, axis=0
    )
    folded = jnp.dot(rows, flat_kv, preferred_element_type=jnp.float32).astype(jnp.bfloat16)
    terms, folded = exchange((("scatter", "dp"), ("columns", "mp")), (branch, folded), 1)
    encoded = (inputs + jnp.sum(terms.astype(jnp.float32), axis=0)).astype(jnp.bfloat16)
    folded = jnp.sum(folded.astype(jnp.float32), axis=0).astype(jnp.bfloat16)
    for bit_index in range(devices_per_kv.bit_length() - 1):
        partner = swapped(folded, "mp", bit_index)
        is_lower = lax.axis_index("mp") // (1 << bit_index) % 2 == 0
        folded = jnp.where(
            is_lower, jnp.concatenate([folded, partner], 1), jnp.concatenate([partner, folded], 1)
        )
    all_encoded, folded = exchange((("chain", "mp"), ("gather", "dp")), (encoded, folded), 2)
    all_encoded = all_encoded.reshape(-1, all_encoded.shape[-1])
    folded = folded.reshape(-1, folded.shape[-1])
    image_rows = all_encoded.shape[0]
    portion = jnp.einsum("rc,kr->ck", folded, all_encoded, preferred_element_type=jnp.float32)
    keys = portion[:HEAD_DIM]
    key_scale = lax.rsqrt(jnp.mean(keys * keys, axis=0, keepdims=True) + 1e-06)
    keys = (keys * key_scale).astype(jnp.bfloat16)
    values = portion[HEAD_DIM:].astype(jnp.bfloat16)
    layout = "dk"
    text_rows = text.shape[1]
    local_heads = q_weight.shape[1] // HEAD_DIM
    queries = jnp.dot(text[0], q_weight, preferred_element_type=jnp.float32).astype(jnp.bfloat16)
    queries = queries.reshape(text_rows, local_heads, HEAD_DIM)
    valid = jnp.arange(image_rows, dtype=jnp.int32) // TILE_TOK < tile_count[0]
    scale = 1.0 / HEAD_DIM**0.5
    block_rows = min(text_rows, 256)
    blocks = queries.reshape(text_rows // block_rows, block_rows, local_heads, HEAD_DIM)
    attended_heads = lax.map(
        lambda block_queries: attend_block(block_queries, keys, values, valid, scale, layout),
        blocks,
    )
    attended_heads = attended_heads.reshape(text_rows, local_heads * HEAD_DIM)
    row_mask = (jnp.arange(text_rows, dtype=jnp.int32) >= text_start[0]).astype(jnp.float32)
    heads_out = (attended_heads * row_mask[:, None]).astype(jnp.bfloat16)
    out = jnp.dot(heads_out, o_weight, preferred_element_type=jnp.float32).astype(jnp.bfloat16)
    out = out.reshape(group_count, text_rows // group_count, out.shape[-1])
    (theirs,) = exchange((("partner", "mp"),), (out,), 3)
    chip_out = out.reshape((group_count // CORES, CORES) + out.shape[1:])
    mine = lax.dynamic_index_in_dim(
        chip_out, lax.axis_index("mp") % CORES, axis=1, keepdims=False
    )
    paired = (mine.astype(jnp.float32) + theirs.astype(jnp.float32)).astype(jnp.bfloat16)
    (terms,) = exchange((("stride", "mp"),), (paired,), 4)
    summed_out = jnp.sum(terms.astype(jnp.float32), axis=0).astype(jnp.bfloat16)
    return summed_out[None]


def erf_gelu(values):
    return 0.5 * values * (1.0 + lax.erf(values * 0.5**0.5))


def fused_kernel(
    image,
    gain,
    fc1,
    fc2,
    projector,
    kv,
    text,
    q_weight,
    o_weight,
    tile_count,
    text_start,
    out,
    up,
    down,
    pixels,
    normed,
    total,
    x_send,
    x_recv,
    z_send,
    z_recv,
    encoded,
    rows_part,
    fold_part,
    fold_0,
    fold_1,
    fold_2,
    fold_3,
    fold_4,
    fold_own,
    folded,
    words,
    staged,
    q_total,
    queries,
    keys,
    values,
    mixed,
    tops,
    sums,
    heads,
    o_part,
    o_0,
    o_1,
    o_2,
    o_3,
    o_4,
    local_sem,
    stage_sem,
    sends,
    recvs,
):
    dp, mp = lax.axis_index("dp"), lax.axis_index("mp")
    core, spot = lax.rem(mp, CORES), lax.div(mp, CORES)
    low, high = lax.rem(spot, 2), lax.div(spot, 2)
    spot_1 = spot + 1 - 2 * low
    spot_2 = spot + 2 - 4 * high
    spot_3 = spot_1 + 2 - 4 * high
    dp_x = dp + 1 - 2 * lax.rem(dp, 2)
    dp_y = dp + 2 - 4 * lax.div(dp, 2)
    pc = {"mp": spot * CORES + 1 - core}
    x1, y1 = {"dp": dp_x}, {"dp": dp_y}
    z1 = {"mp": spot_1 * CORES + core}
    z2 = {"mp": spot_2 * CORES + core}

    barrier = pltpu.get_barrier_semaphore()
    for peer in (pc, x1, y1, z1, z2):
        pl.semaphore_signal(barrier, inc=1, device_id=peer, device_id_type=MESH)

    locals_ = []

    def local(source, target):
        copy = pltpu.make_async_copy(source, target, local_sem.at[len(locals_)])
        copy.start()
        locals_.append(copy)
        return copy

    rows = image.shape[0]
    hidden = fc1.shape[0]
    part_rows = rows_part.shape[0]
    depth = staged.shape[1]
    stages = staged.shape[0]
    half = rows // 2

    kv_parts = kv.shape[1] // depth
    kv_copies = [
        local(kv.at[:, pl.ds(i * depth, depth)], staged.at[i]) for i in range(kv_parts)
    ]
    part_copy = local(
        projector.at[pl.ds(pl.multiple_of(dp * part_rows, part_rows), part_rows)], rows_part
    )

    def q_copy(step):
        slot = lax.rem(step + kv_parts, stages)
        return pltpu.make_async_copy(
            q_weight.at[pl.ds(pl.multiple_of(step * depth, depth), depth)],
            staged.at[slot],
            stage_sem.at[slot],
        )

    def o_copy(step):
        slot = lax.rem(step, stages)
        return pltpu.make_async_copy(
            o_weight.at[:, pl.ds(pl.multiple_of(step * depth, depth), depth)],
            staged.at[slot],
            stage_sem.at[slot],
        )

    text_copy = local(text, words)
    for step in range(stages - kv_parts):
        q_copy(step).start()
    image_copy = local(image, pixels.at[0])
    up_copy = local(fc1, up.at[0, pl.ds(0, hidden)])
    down_copy = local(fc2, down.at[0, pl.ds(0, hidden)])

    pl.semaphore_wait(barrier, 5)

    started = []

    def remote(source, target, peer):
        slot = len(started)
        copy = pltpu.make_async_remote_copy(
            src_ref=source,
            dst_ref=target,
            send_sem=sends.at[slot],
            recv_sem=recvs.at[slot],
            device_id=peer,
            device_id_type=MESH,
        )
        copy.start()
        started.append(copy)
        return copy

    mine, theirs = pl.ds(0, hidden), pl.ds(hidden, hidden)
    image_z = remote(image, pixels.at[2], z1)
    image_x = remote(image, pixels.at[1], x1)
    up_z = remote(fc1, up.at[2, mine], z2)
    down_z = remote(fc2, down.at[2, mine], z2)
    up_y = remote(fc1, up.at[1, mine], y1)
    down_y = remote(fc2, down.at[1, mine], y1)
    up_p = [remote(fc1, up.at[0, theirs], pc)]
    down_p = [remote(fc2, down.at[0, theirs], pc)]

    for copy in kv_copies:
        copy.wait()
    part_copy.wait()
    columns = fold_part.shape[-1]
    per_stage = depth // columns

    def fold_step(head, carry):
        start = pl.multiple_of(lax.rem(head, per_stage) * columns, columns)
        block = staged[lax.div(head, per_stage), :, pl.ds(start, columns)]
        fold_part[lax.div(head, CORES), lax.rem(head, CORES)] = jnp.dot(
            rows_part[...], block, preferred_element_type=jnp.float32
        ).astype(jnp.bfloat16)
        return carry

    lax.fori_loop(0, fold_part.shape[0] * CORES, fold_step, 0)
    fold_p = remote(fold_part.at[:, 1 - core], fold_0, pc)
    for step in range(stages - kv_parts, stages):
        q_copy(step).start()

    text_copy.wait()
    q_steps = q_weight.shape[0] // depth
    q_total[...] = jnp.zeros_like(q_total)

    def q_step(step, carry):
        q_copy(step).wait()
        slot = lax.rem(step + kv_parts, stages)
        q_total[...] += jnp.dot(
            words[:, pl.ds(pl.multiple_of(step * depth, depth), depth)],
            staged[slot],
            preferred_element_type=jnp.float32,
        )

        @pl.when(step + stages < q_steps)
        def _():
            q_copy(step + stages).start()

        return carry

    lax.fori_loop(0, q_steps, q_step, 0)
    text_rows = words.shape[0]
    head_count = q_total.shape[1] // HEAD_DIM
    for head in range(head_count):
        queries[head // 2, pl.ds(head % 2 * text_rows, text_rows)] = q_total[
            :, head * HEAD_DIM : (head + 1) * HEAD_DIM
        ].astype(jnp.bfloat16)
    for step in range(stages):
        o_copy(step).start()

    strip = 32

    def normalise(block):
        def one(step, carry):
            spot_rows = pl.ds(pl.multiple_of(step * strip, strip), strip)
            entry = pixels[block, spot_rows].astype(jnp.float32)
            normed[block, spot_rows] = layer_norm(entry, gain[...]).astype(jnp.bfloat16)
            return carry

        lax.fori_loop(0, rows // strip, one, 0)

    tile = 256

    def mlp(block, first, last, base, stride=1):
        def one(step, carry):
            row = base + step * stride
            inner = lax.dot_general(
                normed[row], up[block], (((1,), (1,)), ((), ())), preferred_element_type=jnp.float32
            )
            inner = erf_gelu(inner).astype(jnp.bfloat16)
            for begin in range(0, total.shape[-1], tile):
                area = pl.ds(begin, tile)
                term = jnp.dot(inner, down[block, :, area], preferred_element_type=jnp.float32)
                if first:
                    total[row, :, area] = term
                else:
                    total[row, :, area] += term
            return carry

        lax.fori_loop(0, last, one, 0)

    image_copy.wait()
    up_copy.wait()
    down_copy.wait()
    normalise(0)
    up_p[0].wait_recv()
    down_p[0].wait_recv()
    mlp(0, True, 1, 0)
    image_z.wait_recv()
    image_d = remote(pixels.at[2], pixels.at[3], x1)
    normalise(2)
    fold_p.wait_recv()
    spots = fold_0.shape[0]

    def fold_pair(index, carry):
        fold_1[lax.div(index, 2), lax.rem(index, 2)] = (
            fold_part[index, core].astype(jnp.float32) + fold_0[index].astype(jnp.float32)
        ).astype(jnp.bfloat16)
        return carry

    lax.fori_loop(0, spots, fold_pair, 0)
    image_x.wait_recv()
    normalise(1)
    mlp(0, True, 2, 1)

    up_z.wait_recv()
    up_d = remote(up.at[2, mine], up.at[3, mine], y1)
    up_p.append(remote(up.at[2, mine], up.at[2, theirs], pc))
    up_y.wait_recv()
    up_p.append(remote(up.at[1, mine], up.at[1, theirs], pc))
    down_y.wait_recv()
    down_p.append(remote(down.at[1, mine], down.at[1, theirs], pc))
    image_d.wait_recv()
    normalise(3)
    mlp(0, True, 1, 3)
    down_z.wait_recv()
    down_d = remote(down.at[2, mine], down.at[3, mine], y1)
    down_p.append(remote(down.at[2, mine], down.at[2, theirs], pc))
    fold_z = remote(fold_1.at[:, 1 - low], fold_2, z1)
    up_p[2].wait_recv()
    down_p[1].wait_recv()
    mlp(1, False, 4, 0)
    up_p[1].wait_recv()
    down_p[2].wait_recv()
    mlp(2, False, 4, 0)
    fold_z.wait_recv()
    for index in range(2):
        fold_3[index] = (
            fold_1[index, low].astype(jnp.float32) + fold_2[index].astype(jnp.float32)
        ).astype(jnp.bfloat16)
    fold_zz = remote(fold_3.at[1 - high], fold_4, z2)
    up_d.wait_recv()
    up_p.append(remote(up.at[3, mine], up.at[3, theirs], pc))
    fold_zz.wait_recv()
    fold_own[...] = (
        fold_3[high].astype(jnp.float32) + fold_4[...].astype(jnp.float32)
    ).astype(jnp.bfloat16)

    def fold_rows(owner):
        return folded.at[pl.ds(pl.multiple_of(owner * part_rows, part_rows), part_rows)]

    fold_local = local(fold_own, fold_rows(dp))
    fold_x = remote(fold_own, fold_rows(dp), x1)
    fold_y = remote(fold_own, fold_rows(dp), y1)
    down_d.wait_recv()
    down_p.append(remote(down.at[3, mine], down.at[3, theirs], pc))
    up_p[3].wait_recv()
    down_p[3].wait_recv()

    def to_x(row, part):
        index = row // 2
        x_send[index, part] = total[row, pl.ds(part * half, half)].astype(jnp.bfloat16)
        return remote(x_send.at[index, part], x_recv.at[index, part], x1)

    mlp(3, False, 1, 1)
    x_copies = {(0, 0): to_x(1, 0)}
    mlp(3, False, 1, 3)
    x_copies[1, 0] = to_x(3, 0)
    x_copies[0, 1] = to_x(1, 1)
    x_copies[1, 1] = to_x(3, 1)
    mlp(3, False, 2, 0, 2)
    fold_x.wait_recv()
    fold_d = remote(fold_rows(dp_x), fold_rows(dp_x), y1)

    order = ((0, 0), (1, 0), (0, 1), (1, 1))
    z_copies = {}
    for index, part in order:
        x_copies[index, part].wait_recv()
        area = pl.ds(part * half, half)
        met = total[2 * index, area] + x_recv[index, part].astype(jnp.float32)
        total[2 * index, area] = met
        z_send[index, part] = met.astype(jnp.bfloat16)
        z_copies[index, part] = remote(z_send.at[index, part], z_recv.at[1 - index, part], z1)
    pairs, onward = {}, {}

    def area_of(core_side, part):
        return pl.ds(core_side * rows + part * half, half)

    def to_partner(unit, part):
        pairs[unit, part] = remote(
            encoded.at[unit, area_of(0, part)], encoded.at[unit, area_of(1, part)], pc
        )

    for index, part in order:
        z_copies[1 - index, part].wait_recv()
        area = pl.ds(part * half, half)
        encoded[index, area_of(0, part)] = (
            pixels[2 * index, area].astype(jnp.float32)
            + total[2 * index, area]
            + z_recv[index, part].astype(jnp.float32)
        ).astype(jnp.bfloat16)
        if index == 0:
            onward[2, part] = remote(
                encoded.at[0, area_of(0, part)], encoded.at[2, area_of(0, part)], z2
            )
        to_partner(index, part)

    fold_local.wait()
    fold_y.wait_recv()
    fold_d.wait_recv()
    scale = 1.0 / HEAD_DIM**0.5
    limit = tile_count[0] * TILE_TOK

    def attend(unit, unit_spot):
        count = 2 * rows
        kv_block = jnp.dot(encoded[unit], folded[...], preferred_element_type=jnp.float32)
        key = kv_block[:, :HEAD_DIM]
        key_scale = lax.rsqrt(jnp.mean(key * key, axis=-1, keepdims=True) + 1e-06)
        keys[...] = (key * key_scale).astype(jnp.bfloat16)
        values[...] = kv_block[:, HEAD_DIM:].astype(jnp.bfloat16)
        place = lax.broadcasted_iota(jnp.int32, (1, count), 1)
        own_base = (unit_spot * CORES + core) * rows
        other_base = (unit_spot * CORES + 1 - core) * rows - rows
        token = place + jnp.where(place < rows, own_base, other_base)
        valid = token < limit

        def one(group, carry):
            scores = (
                lax.dot_general(
                    queries[group],
                    keys[...],
                    (((1,), (1,)), ((), ())),
                    preferred_element_type=jnp.float32,
                )
                * scale
            )
            scores = jnp.where(valid, scores, -1e30)
            top = jnp.max(scores, axis=-1, keepdims=True)
            if unit > 0:
                before = tops[group][:, :1]
                top = jnp.maximum(before, top)
                shrink = jnp.exp(before - top)
            weights = jnp.exp(scores - top)
            weight_sum = jnp.sum(weights, axis=-1, keepdims=True)
            blend = jnp.dot(
                weights.astype(jnp.bfloat16), values[...], preferred_element_type=jnp.float32
            )
            if unit > 0:
                weight_sum += shrink * sums[group][:, :1]
                blend += shrink * mixed[group]
            tops[group] = jnp.broadcast_to(top, tops.shape[1:])
            sums[group] = jnp.broadcast_to(weight_sum, sums.shape[1:])
            mixed[group] = blend
            return carry

        lax.fori_loop(0, queries.shape[0], one, 0)

    for part in range(2):
        pairs[0, part].wait_recv()
    attend(0, spot)

    def pass_on(part):
        onward[2, part].wait_recv()
        onward[3, part] = remote(
            encoded.at[2, area_of(0, part)], encoded.at[3, area_of(0, part)], z1
        )
        to_partner(2, part)

    pass_on(0)
    for part in range(2):
        pairs[1, part].wait_recv()
    attend(1, spot_1)
    pass_on(1)
    for part in range(2):
        pairs[2, part].wait_recv()
    attend(2, spot_2)
    for part in range(2):
        onward[3, part].wait_recv()
        to_partner(3, part)
    for part in range(2):
        pairs[3, part].wait_recv()
    attend(3, spot_3)

    text_at = lax.broadcasted_iota(jnp.int32, (text_rows, 1), 0)
    row_mask = (text_at >= text_start[0]).astype(jnp.float32)
    for head in range(head_count):
        area = pl.ds(head % 2 * text_rows, text_rows)
        heads[:, head * HEAD_DIM : (head + 1) * HEAD_DIM] = (
            mixed[head // 2, area] / sums[head // 2, area][:, :1] * row_mask
        ).astype(jnp.bfloat16)

    steps = o_part.shape[0]
    base = len(started)

    def o_remote(kind, step, source, target, peer):
        return pltpu.make_async_remote_copy(
            src_ref=source,
            dst_ref=target,
            send_sem=sends.at[base + kind * steps + step],
            recv_sem=recvs.at[base + kind * steps + step],
            device_id=peer,
            device_id_type=MESH,
        )

    def o_first(step):
        return o_remote(0, step, o_part.at[step, :, :, 1 - core], o_0.at[step], pc)

    def o_second(step):
        return o_remote(1, step, o_1.at[step, :, 1 - low], o_2.at[step], z1)

    def o_third(step):
        return o_remote(2, step, o_3.at[step, 1 - high], o_4.at[step], z2)

    def meet_first(step):
        o_first(step).wait_recv()
        o_1[step] = (
            o_part[step, :, :, core].astype(jnp.float32) + o_0[step].astype(jnp.float32)
        ).astype(jnp.bfloat16)
        o_second(step).start()

    def meet_second(step):
        o_second(step).wait_recv()
        o_3[step] = (
            o_1[step, :, low].astype(jnp.float32) + o_2[step].astype(jnp.float32)
        ).astype(jnp.bfloat16)
        o_third(step).start()

    def o_step(step, carry):
        o_copy(step).wait()
        slot = lax.rem(step, stages)
        result = jnp.dot(heads[...], staged[slot], preferred_element_type=jnp.float32)
        o_part[step] = result.reshape(o_part.shape[1:]).astype(jnp.bfloat16)
        o_first(step).start()

        @pl.when(step + stages < steps)
        def _():
            o_copy(step + stages).start()

        @pl.when(step > 1)
        def _():
            meet_first(step - 2)

        return carry

    lax.fori_loop(0, steps, o_step, 0)
    meet_first(steps - 2)
    meet_first(steps - 1)

    def second(step, carry):
        meet_second(step)
        return carry

    lax.fori_loop(0, steps, second, 0)

    def third(step, carry):
        o_third(step).wait_recv()
        out[:, pl.ds(pl.multiple_of(step * depth, depth), depth)] = (
            o_3[step, high].astype(jnp.float32) + o_4[step].astype(jnp.float32)
        ).astype(jnp.bfloat16)
        return carry

    lax.fori_loop(0, steps, third, 0)
    for copy in started:
        copy.wait_send()

    def drain(step, carry):
        o_first(step).wait_send()
        o_second(step).wait_send()
        o_third(step).wait_send()
        return carry

    lax.fori_loop(0, steps, drain, 0)


def fused(image, gain, fc1, fc2, projector, kv, text, q_weight, o_weight, tile_count, text_start):
    rows, width = image.shape
    hidden = fc1.shape[0]
    part_rows = projector.shape[0] // lax.axis_size("dp")
    depth = projector.shape[1]
    columns = kv.shape[1] // lax.axis_size("mp")
    text_rows = text.shape[0]
    query_columns = q_weight.shape[1]
    pairs = query_columns // HEAD_DIM // 2
    half = rows // 2
    token_rows = text_rows // lax.axis_size("mp")
    steps = o_weight.shape[1] // depth
    low, wide = jnp.bfloat16, jnp.float32
    copies = 64 + 3 * steps
    scratch = [
        ((4, 2 * hidden, width), low),
        ((4, 2 * hidden, width), low),
        ((4, rows, width), low),
        ((4, rows, width), low),
        ((4, rows, width), wide),
        ((2, 2, half, width), low),
        ((2, 2, half, width), low),
        ((2, 2, half, width), low),
        ((2, 2, half, width), low),
        ((4, 2 * rows, width), low),
        ((part_rows, depth), low),
        ((4, CORES, part_rows, columns), low),
        ((4, part_rows, columns), low),
        ((2, 2, part_rows, columns), low),
        ((2, part_rows, columns), low),
        ((2, part_rows, columns), low),
        ((part_rows, columns), low),
        ((part_rows, columns), low),
        ((width, columns), low),
        (text.shape, low),
        ((4, depth, depth), low),
        ((text_rows, query_columns), wide),
        ((pairs, 2 * text_rows, HEAD_DIM), low),
        ((2 * rows, HEAD_DIM), low),
        ((2 * rows, HEAD_DIM), low),
        ((pairs, 2 * text_rows, HEAD_DIM), wide),
        ((pairs, 2 * text_rows, HEAD_DIM), wide),
        ((pairs, 2 * text_rows, HEAD_DIM), wide),
        ((text_rows, query_columns), low),
        ((steps, 2, 2, CORES, token_rows, depth), low),
        ((steps, 2, 2, token_rows, depth), low),
        ((steps, 2, 2, token_rows, depth), low),
        ((steps, 2, token_rows, depth), low),
        ((steps, 2, token_rows, depth), low),
        ((steps, token_rows, depth), low),
    ]
    vmem, anywhere = pl.BlockSpec(memory_space=pltpu.VMEM), pl.BlockSpec(memory_space=pl.ANY)
    smem = pl.BlockSpec(memory_space=pltpu.SMEM)
    return pl.pallas_call(
        fused_kernel,
        out_shape=jax.ShapeDtypeStruct((token_rows, o_weight.shape[1]), jnp.bfloat16),
        in_specs=[anywhere, vmem] + [anywhere] * 7 + [smem, smem],
        out_specs=vmem,
        scratch_shapes=[pltpu.VMEM(shape, kind) for shape, kind in scratch]
        + [
            pltpu.SemaphoreType.DMA((16,)),
            pltpu.SemaphoreType.DMA((4,)),
            pltpu.SemaphoreType.DMA((copies,)),
            pltpu.SemaphoreType.DMA((copies,)),
        ],
        compiler_params=pltpu.CompilerParams(
            collective_id=7, has_side_effects=True, vmem_limit_bytes=67043328
        ),
        name="fused",
    )(image, gain, fc1, fc2, projector, kv, text, q_weight, o_weight, tile_count, text_start)


def paired_local(
    image,
    ln_gain,
    fc1_weight,
    fc2_weight,
    projector_weight,
    kv_weight,
    text,
    q_weight,
    o_weight,
    tile_count,
    text_start,
):
    return fused(
        image[0],
        ln_gain[None],
        fc1_weight.T,
        fc2_weight,
        projector_weight,
        kv_weight.reshape(kv_weight.shape[0], -1),
        text[0],
        q_weight,
        o_weight,
        tile_count,
        text_start,
    )[None]


def choose(*arrays):
    groups, members = lax.axis_size("dp"), lax.axis_size("mp")
    pairs_of_pairs = groups == members // CORES == 2 * 2
    if pairs_of_pairs and arrays[5].shape[1] == members:
        return paired_local(*arrays)
    return local(*arrays)


def solution(mesh):
    return jax.shard_map(
        choose,
        mesh=mesh,
        in_specs=(
            P("dp", "mp", None),
            P(),
            P(None, ("dp", "mp")),
            P(("dp", "mp"), None),
            P(None, "mp"),
            P("mp", None, None, None),
            P("dp", None, None),
            P(None, "mp"),
            P("mp", None),
            P("dp"),
            P("dp"),
        ),
        out_specs=P("dp", "mp", None),
        check_vma=False,
    )
```

```python
import functools

import jax
import jax.numpy as jnp
from jax import lax
from jax.experimental import pallas as pl
from jax.experimental.pallas import tpu as pltpu
from jax.sharding import PartitionSpec as P

HEAD_DIM = 128
TILE_TOK = 512

MESH = pl.DeviceIdType.MESH
CORES = 2


def count_copies(kind):
    name, axis = kind
    size = lax.axis_size(axis)
    if name == "chain":
        return 2 * (size // CORES - 1) + size // CORES
    if name == "partner":
        return size // CORES
    if name == "stride":
        return size // CORES - 1
    return size - 1


def exchange_kernel(kinds, *refs):
    count = len(kinds)
    sources, results = refs[:count], refs[count : 2 * count]
    local_sem = refs[2 * count]
    sends, recvs = refs[2 * count + 1 : 3 * count + 1], refs[3 * count + 1 :]
    axes = sorted({axis for _, axis in kinds})

    barrier = pltpu.get_barrier_semaphore()
    greeted = 0
    for axis in axes:
        size, me = lax.axis_size(axis), lax.axis_index(axis)
        for step in range(1, size):
            pl.semaphore_signal(
                barrier, inc=1, device_id={axis: lax.rem(me + step, size)}, device_id_type=MESH
            )
        greeted += size - 1
    pl.semaphore_wait(barrier, greeted)

    def remote(op, source, result, slot, axis, peer):
        return pltpu.make_async_remote_copy(
            src_ref=source,
            dst_ref=result,
            send_sem=sends[op].at[slot],
            recv_sem=recvs[op].at[slot],
            device_id={axis: peer},
            device_id_type=MESH,
        )

    simple, chains, locals_ = [], [], []
    for op, (name, axis) in enumerate(kinds):
        size, me = lax.axis_size(axis), lax.axis_index(axis)
        source, result = sources[op], results[op]
        core = lax.rem(me, CORES)
        spot = lax.div(me, CORES)
        partner = me + 1 - 2 * core
        if name == "gather":
            for step in range(1, size):
                copy = remote(op, source, result.at[me], step - 1, axis, lax.rem(me + step, size))
                copy.start()
                simple.append(copy)
            locals_.append(pltpu.make_async_copy(source, result.at[me], local_sem.at[op]))
        elif name == "columns":
            width = result.shape[-1]

            def column(index):
                return source.at[:, pl.ds(pl.multiple_of(index * width, width), width)]

            for step in range(1, size):
                peer = lax.rem(me + step, size)
                copy = remote(op, column(peer), result.at[me], step - 1, axis, peer)
                copy.start()
                simple.append(copy)
            locals_.append(pltpu.make_async_copy(column(me), result.at[me], local_sem.at[op]))
        elif name == "scatter":
            for step in range(1, size):
                peer = lax.rem(me + step, size)
                copy = remote(op, source.at[peer], result.at[me], step - 1, axis, peer)
                copy.start()
                simple.append(copy)
            locals_.append(pltpu.make_async_copy(source.at[me], result.at[me], local_sem.at[op]))
        elif name == "partner":
            for chip in range(size // CORES):
                copy = remote(
                    op, source.at[chip * CORES + 1 - core], result.at[chip], chip, axis, partner
                )
                copy.start()
                simple.append(copy)
        elif name == "stride":
            chips = size // CORES
            for step in range(1, chips):
                other = lax.rem(spot + step, chips)
                copy = remote(
                    op, source.at[other], result.at[spot], step - 1, axis, other * CORES + core
                )
                copy.start()
                simple.append(copy)
            locals_.append(pltpu.make_async_copy(source.at[spot], result.at[spot], local_sem.at[op]))
        else:
            chains.append((op, axis, size // CORES, me, core, spot, partner, source, result))
    for copy in locals_:
        copy.start()

    def hop(chain, source, block, slot, peer):
        op, axis, result = chain[0], chain[1], chain[-1]
        return remote(op, source, result.at[block], slot, axis, peer)

    for chain in chains:
        op, axis, chips, me, core, spot, partner, source, result = chain

        @pl.when(spot + 1 < chips)
        def _():
            hop(chain, source, me, 0, me + CORES).start()

        @pl.when(spot > 0)
        def _():
            hop(chain, source, me, chips - 1, me - CORES).start()

    for chain in chains:
        op, axis, chips, me, core, spot, partner, source, result = chain
        hop(chain, source, me, 2 * (chips - 1), partner).start()
        pltpu.make_async_copy(source, result.at[me], local_sem.at[op]).start()
    for step in range(1, max([chain[2] for chain in chains], default=0)):
        for chain in chains:
            op, axis, chips, me, core, spot, partner, source, result = chain
            for sign, base in ((1, 0), (-1, chips - 1)):
                origin_spot = spot - sign * step
                here = (origin_spot >= 0) & (origin_spot < chips)
                onward = (spot + sign >= 0) & (spot + sign < chips)
                block = me - sign * step * CORES

                @pl.when(here)
                def _():
                    held = result.at[block]
                    hop(chain, held, block, base + step - 1, me).wait_recv()

                    @pl.when(onward)
                    def _():
                        hop(chain, held, block, base + step, me + sign * CORES).start()

                    slot = 2 * (chips - 1) + lax.rem(origin_spot - spot + chips, chips)
                    hop(chain, held, block, slot, partner).start()

    for chain in chains:
        op, axis, chips, me, core, spot, partner, source, result = chain
        for step in range(chips):
            for_spot = lax.rem(spot + step, chips)
            block = for_spot * CORES + core
            theirs = for_spot * CORES + 1 - core
            slot = 2 * (chips - 1) + step
            hop(chain, result.at[block], block, slot, partner).wait_send()
            hop(chain, result.at[theirs], theirs, slot, partner).wait_recv()
        for step in range(chips - 1):
            for sign, base in ((1, 0), (-1, chips - 1)):
                origin_spot = spot - sign * step
                sent = (
                    (origin_spot >= 0)
                    & (origin_spot < chips)
                    & (spot + sign >= 0)
                    & (spot + sign < chips)
                )
                block = me - sign * step * CORES

                @pl.when(sent)
                def _():
                    hop(chain, source, block, base + step, partner).wait_send()

        pltpu.make_async_copy(source, result.at[me], local_sem.at[op]).wait()
    for copy in simple:
        copy.wait()
    for copy in locals_:
        copy.wait()


def exchange(kinds, arrays, number):
    kinds = tuple(kinds)
    shapes = []
    for (name, axis), array in zip(kinds, arrays):
        size = lax.axis_size(axis)
        if name in ("gather", "chain"):
            shape = (size,) + array.shape
        elif name == "columns":
            shape = (size, array.shape[0], array.shape[1] // size)
        elif name == "scatter":
            shape = array.shape
        else:
            shape = (size // CORES,) + array.shape[1:]
        shapes.append(jax.ShapeDtypeStruct(shape, array.dtype))
    sems = [pltpu.SemaphoreType.DMA((count_copies(kind),)) for kind in kinds]
    return pl.pallas_call(
        functools.partial(exchange_kernel, kinds),
        out_shape=shapes,
        in_specs=[pl.BlockSpec(memory_space=pl.ANY)] * len(kinds),
        out_specs=[pl.BlockSpec(memory_space=pl.ANY)] * len(kinds),
        scratch_shapes=[pltpu.SemaphoreType.DMA((len(kinds),))] + sems + sems,
        compiler_params=pltpu.CompilerParams(collective_id=number, has_side_effects=True),
        name="exchange",
    )(*arrays)


def swapped(block, axis, bit):
    count = lax.axis_size(axis)
    route = []
    for low in range(count):
        high = low | 1 << bit
        if high != low and high < count:
            route += [(low, high), (high, low)]
    return lax.ppermute(block, axis, route)


def layer_norm(values, gain):
    center = values - jnp.mean(values, axis=-1, keepdims=True)
    spread = jnp.mean(center * center, axis=-1, keepdims=True)
    return center * lax.rsqrt(spread + 1e-05) * gain


def attend_block(block_queries, keys, values, valid, scale, layout):
    scores = (
        jnp.einsum(
            "thd," + layout + "->htk", block_queries, keys, preferred_element_type=jnp.float32
        )
        * scale
    )
    scores = jnp.where(valid[None, None, :], scores, -1e30)
    top = jnp.max(scores, axis=-1, keepdims=True)
    weights = jnp.exp(scores - top)
    probs = (weights / jnp.sum(weights, axis=-1, keepdims=True)).astype(jnp.bfloat16)
    return jnp.einsum("htk," + layout + "->thd", probs, values, preferred_element_type=jnp.float32)


def local(
    image,
    ln_gain,
    fc1_weight,
    fc2_weight,
    projector_weight,
    kv_weight,
    text,
    q_weight,
    o_weight,
    tile_count,
    text_start,
):
    inputs = image[0].astype(jnp.float32)
    group_count = lax.axis_size("mp")
    normed = layer_norm(inputs, ln_gain).astype(jnp.bfloat16)
    up, down, all_normed = exchange(
        (("chain", "mp"), ("chain", "mp"), ("gather", "dp")), (fc1_weight.T, fc2_weight, normed), 0
    )
    up = up.reshape(-1, up.shape[-1])
    down = down.reshape(-1, down.shape[-1])
    all_normed = all_normed.reshape(-1, all_normed.shape[-1])
    hidden = jax.nn.gelu(
        lax.dot_general(
            all_normed, up, (((1,), (1,)), ((), ())), preferred_element_type=jnp.float32
        ),
        approximate=False,
    ).astype(jnp.bfloat16)
    branch = jnp.dot(hidden, down, preferred_element_type=jnp.float32).astype(jnp.bfloat16)
    branch = branch.reshape((lax.axis_size("dp"),) + inputs.shape)

    kv_count = kv_weight.shape[1]
    devices_per_kv = group_count // kv_count
    kv_columns = kv_count * 2 * HEAD_DIM
    flat_kv = kv_weight.reshape(kv_weight.shape[0], kv_columns)
    row_count = projector_weight.shape[0] // lax.axis_size("dp")
    rows = lax.dynamic_slice_in_dim(
        projector_weight, lax.axis_index("dp") * row_count, row_count, axis=0
    )
    folded = jnp.dot(rows, flat_kv, preferred_element_type=jnp.float32).astype(jnp.bfloat16)
    terms, folded = exchange((("scatter", "dp"), ("columns", "mp")), (branch, folded), 1)
    encoded = (inputs + jnp.sum(terms.astype(jnp.float32), axis=0)).astype(jnp.bfloat16)
    folded = jnp.sum(folded.astype(jnp.float32), axis=0).astype(jnp.bfloat16)
    for bit_index in range(devices_per_kv.bit_length() - 1):
        partner = swapped(folded, "mp", bit_index)
        is_lower = lax.axis_index("mp") // (1 << bit_index) % 2 == 0
        folded = jnp.where(
            is_lower, jnp.concatenate([folded, partner], 1), jnp.concatenate([partner, folded], 1)
        )
    all_encoded, folded = exchange((("chain", "mp"), ("gather", "dp")), (encoded, folded), 2)
    all_encoded = all_encoded.reshape(-1, all_encoded.shape[-1])
    folded = folded.reshape(-1, folded.shape[-1])
    image_rows = all_encoded.shape[0]
    portion = jnp.einsum("rc,kr->ck", folded, all_encoded, preferred_element_type=jnp.float32)
    keys = portion[:HEAD_DIM]
    key_scale = lax.rsqrt(jnp.mean(keys * keys, axis=0, keepdims=True) + 1e-06)
    keys = (keys * key_scale).astype(jnp.bfloat16)
    values = portion[HEAD_DIM:].astype(jnp.bfloat16)
    layout = "dk"
    text_rows = text.shape[1]
    local_heads = q_weight.shape[1] // HEAD_DIM
    queries = jnp.dot(text[0], q_weight, preferred_element_type=jnp.float32).astype(jnp.bfloat16)
    queries = queries.reshape(text_rows, local_heads, HEAD_DIM)
    valid = jnp.arange(image_rows, dtype=jnp.int32) // TILE_TOK < tile_count[0]
    scale = 1.0 / HEAD_DIM**0.5
    block_rows = min(text_rows, 256)
    blocks = queries.reshape(text_rows // block_rows, block_rows, local_heads, HEAD_DIM)
    attended_heads = lax.map(
        lambda block_queries: attend_block(block_queries, keys, values, valid, scale, layout),
        blocks,
    )
    attended_heads = attended_heads.reshape(text_rows, local_heads * HEAD_DIM)
    row_mask = (jnp.arange(text_rows, dtype=jnp.int32) >= text_start[0]).astype(jnp.float32)
    heads_out = (attended_heads * row_mask[:, None]).astype(jnp.bfloat16)
    out = jnp.dot(heads_out, o_weight, preferred_element_type=jnp.float32).astype(jnp.bfloat16)
    out = out.reshape(group_count, text_rows // group_count, out.shape[-1])
    (theirs,) = exchange((("partner", "mp"),), (out,), 3)
    chip_out = out.reshape((group_count // CORES, CORES) + out.shape[1:])
    mine = lax.dynamic_index_in_dim(
        chip_out, lax.axis_index("mp") % CORES, axis=1, keepdims=False
    )
    paired = (mine.astype(jnp.float32) + theirs.astype(jnp.float32)).astype(jnp.bfloat16)
    (terms,) = exchange((("stride", "mp"),), (paired,), 4)
    summed_out = jnp.sum(terms.astype(jnp.float32), axis=0).astype(jnp.bfloat16)
    return summed_out[None]


def erf_gelu(values):
    return 0.5 * values * (1.0 + lax.erf(values * 0.5**0.5))


def fused_kernel(
    image,
    gain,
    fc1,
    fc2,
    projector,
    kv,
    text,
    q_weight,
    o_weight,
    tile_count,
    text_start,
    out,
    up,
    down,
    pixels,
    normed,
    total,
    x_send,
    x_recv,
    z_send,
    z_recv,
    encoded,
    rows_part,
    kv_raw,
    kv_flat,
    fold_part,
    fold_0,
    fold_1,
    fold_2,
    fold_3,
    fold_4,
    fold_own,
    folded,
    words,
    staged,
    q_total,
    queries,
    keys,
    values,
    mixed,
    tops,
    sums,
    heads,
    o_part,
    o_0,
    o_1,
    o_2,
    o_3,
    o_4,
    local_sem,
    stage_sem,
    sends,
    recvs,
):
    dp, mp = lax.axis_index("dp"), lax.axis_index("mp")
    core, spot = lax.rem(mp, CORES), lax.div(mp, CORES)
    low, high = lax.rem(spot, 2), lax.div(spot, 2)
    spot_1 = spot + 1 - 2 * low
    spot_2 = spot + 2 - 4 * high
    spot_3 = spot_1 + 2 - 4 * high
    dp_x = dp + 1 - 2 * lax.rem(dp, 2)
    dp_y = dp + 2 - 4 * lax.div(dp, 2)
    pc = {"mp": spot * CORES + 1 - core}
    x1, y1 = {"dp": dp_x}, {"dp": dp_y}
    z1 = {"mp": spot_1 * CORES + core}
    z2 = {"mp": spot_2 * CORES + core}

    barrier = pltpu.get_barrier_semaphore()
    for peer in (pc, x1, y1, z1, z2):
        pl.semaphore_signal(barrier, inc=1, device_id=peer, device_id_type=MESH)

    locals_ = []

    def local(source, target):
        copy = pltpu.make_async_copy(source, target, local_sem.at[len(locals_)])
        copy.start()
        locals_.append(copy)
        return copy

    rows = image.shape[0]
    hidden = fc1.shape[0]
    part_rows = rows_part.shape[0]
    depth = staged.shape[1]
    stages = staged.shape[0]
    half = rows // 2

    def q_copy(step):
        slot = lax.rem(step, stages)
        return pltpu.make_async_copy(
            q_weight.at[pl.ds(pl.multiple_of(step * depth, depth), depth)],
            staged.at[slot],
            stage_sem.at[slot],
        )

    def o_copy(step):
        slot = lax.rem(step, stages)
        return pltpu.make_async_copy(
            o_weight.at[:, pl.ds(pl.multiple_of(step * depth, depth), depth)],
            staged.at[slot],
            stage_sem.at[slot],
        )

    image_copy = local(image, pixels.at[0])
    up_copy = local(fc1, up.at[0, pl.ds(0, hidden)])
    down_copy = local(fc2, down.at[0, pl.ds(0, hidden)])
    text_copy = local(text, words)
    for step in range(stages):
        q_copy(step).start()
    kv_copy = local(kv, kv_raw)
    part_copy = local(
        projector.at[pl.ds(pl.multiple_of(dp * part_rows, part_rows), part_rows)], rows_part
    )

    pl.semaphore_wait(barrier, 5)

    started = []

    def remote(source, target, peer):
        slot = len(started)
        copy = pltpu.make_async_remote_copy(
            src_ref=source,
            dst_ref=target,
            send_sem=sends.at[slot],
            recv_sem=recvs.at[slot],
            device_id=peer,
            device_id_type=MESH,
        )
        copy.start()
        started.append(copy)
        return copy

    mine, theirs = pl.ds(0, hidden), pl.ds(hidden, hidden)
    halves = [pl.ds(part * half, half) for part in range(2)]
    bits = [pl.ds(part * (hidden // 2), hidden // 2) for part in range(2)]
    image_z = [remote(image.at[area], pixels.at[2, area], z1) for area in halves]
    image_x = remote(image, pixels.at[1], x1)
    up_z = [remote(fc1.at[area], up.at[2, area], z2) for area in bits]
    down_z = [remote(fc2.at[area], down.at[2, area], z2) for area in bits]
    up_y = remote(fc1, up.at[1, mine], y1)
    down_y = remote(fc2, down.at[1, mine], y1)
    up_p = {0: remote(fc1, up.at[0, theirs], pc)}
    down_p = {0: remote(fc2, down.at[0, theirs], pc)}

    text_copy.wait()
    q_steps = q_weight.shape[0] // depth
    q_total[...] = jnp.zeros_like(q_total)

    def q_step(step, carry):
        q_copy(step).wait()
        q_total[...] += jnp.dot(
            words[:, pl.ds(pl.multiple_of(step * depth, depth), depth)],
            staged[lax.rem(step, stages)],
            preferred_element_type=jnp.float32,
        )

        @pl.when(step + stages < q_steps)
        def _():
            q_copy(step + stages).start()

        return carry

    lax.fori_loop(0, q_steps, q_step, 0)
    text_rows = words.shape[0]
    head_count = q_total.shape[1] // HEAD_DIM
    for head in range(head_count):
        queries[head // 2, pl.ds(head % 2 * text_rows, text_rows)] = q_total[
            :, head * HEAD_DIM : (head + 1) * HEAD_DIM
        ].astype(jnp.bfloat16)

    strip = 32

    def normalise(block):
        def one(step, carry):
            spot_rows = pl.ds(pl.multiple_of(step * strip, strip), strip)
            entry = pixels[block, spot_rows].astype(jnp.float32)
            normed[block, spot_rows] = layer_norm(entry, gain[...]).astype(jnp.bfloat16)
            return carry

        lax.fori_loop(0, rows // strip, one, 0)

    tile = 256

    def mlp(block, first, last, base, stride=1):
        def one(step, carry):
            row = base + step * stride
            inner = lax.dot_general(
                normed[row], up[block], (((1,), (1,)), ((), ())), preferred_element_type=jnp.float32
            )
            inner = erf_gelu(inner).astype(jnp.bfloat16)
            for begin in range(0, total.shape[-1], tile):
                area = pl.ds(begin, tile)
                term = jnp.dot(inner, down[block, :, area], preferred_element_type=jnp.float32)
                if first:
                    total[row, :, area] = term
                else:
                    total[row, :, area] += term
            return carry

        lax.fori_loop(0, last, one, 0)

    image_copy.wait()
    up_copy.wait()
    down_copy.wait()
    normalise(0)
    up_p[0].wait_recv()
    down_p[0].wait_recv()
    mlp(0, True, 1, 0)
    kv_copy.wait()
    flat = 16

    def flatten(step, carry):
        area = pl.ds(pl.multiple_of(step * flat, flat), flat)
        kv_flat[area] = kv_raw[area].reshape(flat, kv_flat.shape[1])
        return carry

    lax.fori_loop(0, kv_flat.shape[0] // flat, flatten, 0)
    part_copy.wait()
    columns = fold_part.shape[-1]

    def fold_step(head, carry):
        block = kv_flat[:, pl.ds(pl.multiple_of(head * columns, columns), columns)]
        fold_part[lax.div(head, CORES), lax.rem(head, CORES)] = jnp.dot(
            rows_part[...], block, preferred_element_type=jnp.float32
        ).astype(jnp.bfloat16)
        return carry

    lax.fori_loop(0, fold_part.shape[0] * CORES, fold_step, 0)
    fold_p = remote(fold_part.at[:, 1 - core], fold_0, pc)
    for step in range(stages):
        o_copy(step).start()
    image_x.wait_recv()
    normalise(1)
    mlp(0, True, 1, 1)
    up_y.wait_recv()
    up_p[1] = remote(up.at[1, mine], up.at[1, theirs], pc)
    down_y.wait_recv()
    down_p[1] = remote(down.at[1, mine], down.at[1, theirs], pc)
    up_d, down_d = [], []
    for part, copy in enumerate(up_z):
        copy.wait_recv()
        up_d.append(remote(up.at[2, bits[part]], up.at[3, bits[part]], y1))
    up_p[2] = remote(up.at[2, mine], up.at[2, theirs], pc)
    image_d = []
    image_z[0].wait_recv()
    image_d.append(remote(pixels.at[2, halves[0]], pixels.at[3, halves[0]], x1))
    up_p[1].wait_recv()
    down_p[1].wait_recv()
    mlp(1, False, 2, 0)
    image_z[1].wait_recv()
    image_d.append(remote(pixels.at[2, halves[1]], pixels.at[3, halves[1]], x1))
    normalise(2)
    for part, copy in enumerate(down_z):
        copy.wait_recv()
        down_d.append(remote(down.at[2, bits[part]], down.at[3, bits[part]], y1))
    down_p[2] = remote(down.at[2, mine], down.at[2, theirs], pc)
    fold_p.wait_recv()
    spots = fold_0.shape[0]

    def fold_pair(index, carry):
        fold_1[lax.div(index, 2), lax.rem(index, 2)] = (
            fold_part[index, core].astype(jnp.float32) + fold_0[index].astype(jnp.float32)
        ).astype(jnp.bfloat16)
        return carry

    lax.fori_loop(0, spots, fold_pair, 0)
    fold_z = remote(fold_1.at[:, 1 - low], fold_2, z1)
    mlp(0, True, 1, 2)
    mlp(1, False, 1, 2)
    up_p[2].wait_recv()
    down_p[2].wait_recv()
    mlp(2, False, 3, 0)
    for copy in image_d:
        copy.wait_recv()
    normalise(3)
    for copy in up_d:
        copy.wait_recv()
    up_p[3] = remote(up.at[3, mine], up.at[3, theirs], pc)
    mlp(0, True, 1, 3)
    mlp(1, False, 1, 3)
    mlp(2, False, 1, 3)
    for copy in down_d:
        copy.wait_recv()
    down_p[3] = remote(down.at[3, mine], down.at[3, theirs], pc)
    up_p[3].wait_recv()
    down_p[3].wait_recv()

    def to_x(row, part):
        index = row // 2
        x_send[index, part] = total[row, pl.ds(part * half, half)].astype(jnp.bfloat16)
        return remote(x_send.at[index, part], x_recv.at[index, part], x1)

    mlp(3, False, 1, 1)
    x_copies = {(0, 0): to_x(1, 0)}
    mlp(3, False, 1, 3)
    x_copies[1, 0] = to_x(3, 0)
    x_copies[0, 1] = to_x(1, 1)
    x_copies[1, 1] = to_x(3, 1)
    mlp(3, False, 2, 0, 2)
    fold_z.wait_recv()
    for index in range(2):
        fold_3[index] = (
            fold_1[index, low].astype(jnp.float32) + fold_2[index].astype(jnp.float32)
        ).astype(jnp.bfloat16)
    fold_zz = remote(fold_3.at[1 - high], fold_4, z2)

    def fold_rows(owner):
        return folded.at[pl.ds(pl.multiple_of(owner * part_rows, part_rows), part_rows)]

    order = ((0, 0), (1, 0), (0, 1), (1, 1))
    z_copies = {}
    for number, (index, part) in enumerate(order):
        x_copies[index, part].wait_recv()
        area = pl.ds(part * half, half)
        met = total[2 * index, area] + x_recv[index, part].astype(jnp.float32)
        total[2 * index, area] = met
        z_send[index, part] = met.astype(jnp.bfloat16)
        z_copies[index, part] = remote(z_send.at[index, part], z_recv.at[1 - index, part], z1)
        if number == 0:
            fold_zz.wait_recv()
            fold_own[...] = (
                fold_3[high].astype(jnp.float32) + fold_4[...].astype(jnp.float32)
            ).astype(jnp.bfloat16)
            fold_local = local(fold_own, fold_rows(dp))
            fold_y = remote(fold_own, fold_rows(dp), y1)
            fold_x = remote(fold_own, fold_rows(dp), x1)
    pairs, onward = {}, {}

    def area_of(core_side, part):
        return pl.ds(core_side * rows + part * half, half)

    def to_partner(unit, part):
        pairs[unit, part] = remote(
            encoded.at[unit, area_of(0, part)], encoded.at[unit, area_of(1, part)], pc
        )

    for index, part in order:
        z_copies[1 - index, part].wait_recv()
        area = pl.ds(part * half, half)
        encoded[index, area_of(0, part)] = (
            pixels[2 * index, area].astype(jnp.float32)
            + total[2 * index, area]
            + z_recv[index, part].astype(jnp.float32)
        ).astype(jnp.bfloat16)
        if index == 0:
            onward[2, part] = remote(
                encoded.at[0, area_of(0, part)], encoded.at[2, area_of(0, part)], z2
            )
        to_partner(index, part)

    fold_local.wait()
    fold_x.wait_recv()
    fold_d = remote(fold_rows(dp_x), fold_rows(dp_x), y1)
    fold_y.wait_recv()
    fold_d.wait_recv()
    scale = 1.0 / HEAD_DIM**0.5
    limit = tile_count[0] * TILE_TOK

    def attend(unit, unit_spot):
        count = 2 * rows
        kv_block = jnp.dot(encoded[unit], folded[...], preferred_element_type=jnp.float32)
        key = kv_block[:, :HEAD_DIM]
        key_scale = lax.rsqrt(jnp.mean(key * key, axis=-1, keepdims=True) + 1e-06)
        keys[...] = (key * key_scale).astype(jnp.bfloat16)
        values[...] = kv_block[:, HEAD_DIM:].astype(jnp.bfloat16)
        place = lax.broadcasted_iota(jnp.int32, (1, count), 1)
        own_base = (unit_spot * CORES + core) * rows
        other_base = (unit_spot * CORES + 1 - core) * rows - rows
        token = place + jnp.where(place < rows, own_base, other_base)
        valid = token < limit

        def one(group, carry):
            scores = (
                lax.dot_general(
                    queries[group],
                    keys[...],
                    (((1,), (1,)), ((), ())),
                    preferred_element_type=jnp.float32,
                )
                * scale
            )
            scores = jnp.where(valid, scores, -1e30)
            top = jnp.max(scores, axis=-1, keepdims=True)
            if unit > 0:
                before = tops[group][:, :1]
                top = jnp.maximum(before, top)
                shrink = jnp.exp(before - top)
            weights = jnp.exp(scores - top)
            weight_sum = jnp.sum(weights, axis=-1, keepdims=True)
            blend = jnp.dot(
                weights.astype(jnp.bfloat16), values[...], preferred_element_type=jnp.float32
            )
            if unit > 0:
                weight_sum += shrink * sums[group][:, :1]
                blend += shrink * mixed[group]
            tops[group] = jnp.broadcast_to(top, tops.shape[1:])
            sums[group] = jnp.broadcast_to(weight_sum, sums.shape[1:])
            mixed[group] = blend
            return carry

        lax.fori_loop(0, queries.shape[0], one, 0)

    for part in range(2):
        pairs[0, part].wait_recv()
    attend(0, spot)

    def pass_on(part):
        onward[2, part].wait_recv()
        onward[3, part] = remote(
            encoded.at[2, area_of(0, part)], encoded.at[3, area_of(0, part)], z1
        )
        to_partner(2, part)

    pass_on(0)
    for part in range(2):
        pairs[1, part].wait_recv()
    attend(1, spot_1)
    pass_on(1)
    for part in range(2):
        pairs[2, part].wait_recv()
    attend(2, spot_2)
    for part in range(2):
        onward[3, part].wait_recv()
        to_partner(3, part)
    for part in range(2):
        pairs[3, part].wait_recv()
    attend(3, spot_3)

    text_at = lax.broadcasted_iota(jnp.int32, (text_rows, 1), 0)
    row_mask = (text_at >= text_start[0]).astype(jnp.float32)
    for head in range(head_count):
        area = pl.ds(head % 2 * text_rows, text_rows)
        heads[:, head * HEAD_DIM : (head + 1) * HEAD_DIM] = (
            mixed[head // 2, area] / sums[head // 2, area][:, :1] * row_mask
        ).astype(jnp.bfloat16)

    steps = o_part.shape[0]
    base = len(started)

    def o_remote(kind, step, source, target, peer):
        return pltpu.make_async_remote_copy(
            src_ref=source,
            dst_ref=target,
            send_sem=sends.at[base + kind * steps + step],
            recv_sem=recvs.at[base + kind * steps + step],
            device_id=peer,
            device_id_type=MESH,
        )

    def o_first(step):
        return o_remote(0, step, o_part.at[step, :, :, 1 - core], o_0.at[step], pc)

    def o_second(step):
        return o_remote(1, step, o_1.at[step, :, 1 - low], o_2.at[step], z1)

    def o_third(step):
        return o_remote(2, step, o_3.at[step, 1 - high], o_4.at[step], z2)

    def meet_first(step):
        o_first(step).wait_recv()
        o_1[step] = (
            o_part[step, :, :, core].astype(jnp.float32) + o_0[step].astype(jnp.float32)
        ).astype(jnp.bfloat16)
        o_second(step).start()

    def meet_second(step):
        o_second(step).wait_recv()
        o_3[step] = (
            o_1[step, :, low].astype(jnp.float32) + o_2[step].astype(jnp.float32)
        ).astype(jnp.bfloat16)
        o_third(step).start()

    def o_step(step, carry):
        o_copy(step).wait()
        slot = lax.rem(step, stages)
        result = jnp.dot(heads[...], staged[slot], preferred_element_type=jnp.float32)
        o_part[step] = result.reshape(o_part.shape[1:]).astype(jnp.bfloat16)
        o_first(step).start()

        @pl.when(step + stages < steps)
        def _():
            o_copy(step + stages).start()

        @pl.when(step > 1)
        def _():
            meet_first(step - 2)

        return carry

    lax.fori_loop(0, steps, o_step, 0)
    meet_first(steps - 2)
    meet_first(steps - 1)

    def second(step, carry):
        meet_second(step)
        return carry

    lax.fori_loop(0, steps, second, 0)

    def third(step, carry):
        o_third(step).wait_recv()
        out[:, pl.ds(pl.multiple_of(step * depth, depth), depth)] = (
            o_3[step, high].astype(jnp.float32) + o_4[step].astype(jnp.float32)
        ).astype(jnp.bfloat16)
        return carry

    lax.fori_loop(0, steps, third, 0)
    for copy in started:
        copy.wait_send()

    def drain(step, carry):
        o_first(step).wait_send()
        o_second(step).wait_send()
        o_third(step).wait_send()
        return carry

    lax.fori_loop(0, steps, drain, 0)


def fused(image, gain, fc1, fc2, projector, kv, text, q_weight, o_weight, tile_count, text_start):
    rows, width = image.shape
    hidden = fc1.shape[0]
    part_rows = projector.shape[0] // lax.axis_size("dp")
    depth = projector.shape[1]
    kv_columns = kv.shape[1] * kv.shape[2] * kv.shape[3]
    columns = kv_columns // lax.axis_size("mp")
    text_rows = text.shape[0]
    query_columns = q_weight.shape[1]
    pairs = query_columns // HEAD_DIM // 2
    half = rows // 2
    token_rows = text_rows // lax.axis_size("mp")
    steps = o_weight.shape[1] // depth
    low, wide = jnp.bfloat16, jnp.float32
    copies = 64 + 3 * steps
    scratch = [
        ((4, 2 * hidden, width), low),
        ((4, 2 * hidden, width), low),
        ((4, rows, width), low),
        ((4, rows, width), low),
        ((4, rows, width), wide),
        ((2, 2, half, width), low),
        ((2, 2, half, width), low),
        ((2, 2, half, width), low),
        ((2, 2, half, width), low),
        ((4, 2 * rows, width), low),
        ((part_rows, depth), low),
        (kv.shape, low),
        ((kv.shape[0], kv_columns), low),
        ((4, CORES, part_rows, columns), low),
        ((4, part_rows, columns), low),
        ((2, 2, part_rows, columns), low),
        ((2, part_rows, columns), low),
        ((2, part_rows, columns), low),
        ((part_rows, columns), low),
        ((part_rows, columns), low),
        ((width, columns), low),
        (text.shape, low),
        ((4, depth, depth), low),
        ((text_rows, query_columns), wide),
        ((pairs, 2 * text_rows, HEAD_DIM), low),
        ((2 * rows, HEAD_DIM), low),
        ((2 * rows, HEAD_DIM), low),
        ((pairs, 2 * text_rows, HEAD_DIM), wide),
        ((pairs, 2 * text_rows, HEAD_DIM), wide),
        ((pairs, 2 * text_rows, HEAD_DIM), wide),
        ((text_rows, query_columns), low),
        ((steps, 2, 2, CORES, token_rows, depth), low),
        ((steps, 2, 2, token_rows, depth), low),
        ((steps, 2, 2, token_rows, depth), low),
        ((steps, 2, token_rows, depth), low),
        ((steps, 2, token_rows, depth), low),
        ((steps, token_rows, depth), low),
    ]
    vmem, anywhere = pl.BlockSpec(memory_space=pltpu.VMEM), pl.BlockSpec(memory_space=pl.ANY)
    smem = pl.BlockSpec(memory_space=pltpu.SMEM)
    return pl.pallas_call(
        fused_kernel,
        out_shape=jax.ShapeDtypeStruct((token_rows, o_weight.shape[1]), jnp.bfloat16),
        in_specs=[anywhere, vmem] + [anywhere] * 7 + [smem, smem],
        out_specs=vmem,
        scratch_shapes=[pltpu.VMEM(shape, kind) for shape, kind in scratch]
        + [
            pltpu.SemaphoreType.DMA((16,)),
            pltpu.SemaphoreType.DMA((4,)),
            pltpu.SemaphoreType.DMA((copies,)),
            pltpu.SemaphoreType.DMA((copies,)),
        ],
        compiler_params=pltpu.CompilerParams(
            collective_id=7, has_side_effects=True, vmem_limit_bytes=67043328
        ),
        name="fused",
    )(image, gain, fc1, fc2, projector, kv, text, q_weight, o_weight, tile_count, text_start)


def paired_local(
    image,
    ln_gain,
    fc1_weight,
    fc2_weight,
    projector_weight,
    kv_weight,
    text,
    q_weight,
    o_weight,
    tile_count,
    text_start,
):
    return fused(
        image[0],
        ln_gain,
        fc1_weight.T,
        fc2_weight,
        projector_weight,
        kv_weight,
        text[0],
        q_weight,
        o_weight,
        tile_count,
        text_start,
    )[None]


def choose(*arrays):
    groups, members = lax.axis_size("dp"), lax.axis_size("mp")
    pairs_of_pairs = groups == members // CORES == 2 * 2
    if pairs_of_pairs and arrays[5].shape[1] == members:
        return paired_local(*arrays)
    return local(*arrays)


def solution(mesh):
    return jax.shard_map(
        choose,
        mesh=mesh,
        in_specs=(
            P("dp", "mp", None),
            P(),
            P(None, ("dp", "mp")),
            P(("dp", "mp"), None),
            P(None, "mp"),
            P("mp", None, None, None),
            P("dp", None, None),
            P(None, "mp"),
            P("mp", None),
            P("dp"),
            P("dp"),
        ),
        out_specs=P("dp", "mp", None),
        check_vma=False,
    )
```

```python
import functools

import jax
import jax.numpy as jnp
from jax import lax
from jax.experimental import pallas as pl
from jax.experimental.pallas import tpu as pltpu
from jax.sharding import PartitionSpec as P

HEAD_DIM = 128
TILE_TOK = 512

MESH = pl.DeviceIdType.MESH
CORES = 2


def count_copies(kind):
    name, axis = kind
    size = lax.axis_size(axis)
    if name == "chain":
        return 2 * (size // CORES - 1) + size // CORES
    if name == "partner":
        return size // CORES
    if name == "stride":
        return size // CORES - 1
    return size - 1


def exchange_kernel(kinds, *refs):
    count = len(kinds)
    sources, results = refs[:count], refs[count : 2 * count]
    local_sem = refs[2 * count]
    sends, recvs = refs[2 * count + 1 : 3 * count + 1], refs[3 * count + 1 :]
    axes = sorted({axis for _, axis in kinds})

    barrier = pltpu.get_barrier_semaphore()
    greeted = 0
    for axis in axes:
        size, me = lax.axis_size(axis), lax.axis_index(axis)
        for step in range(1, size):
            pl.semaphore_signal(
                barrier, inc=1, device_id={axis: lax.rem(me + step, size)}, device_id_type=MESH
            )
        greeted += size - 1
    pl.semaphore_wait(barrier, greeted)

    def remote(op, source, result, slot, axis, peer):
        return pltpu.make_async_remote_copy(
            src_ref=source,
            dst_ref=result,
            send_sem=sends[op].at[slot],
            recv_sem=recvs[op].at[slot],
            device_id={axis: peer},
            device_id_type=MESH,
        )

    simple, chains, locals_ = [], [], []
    for op, (name, axis) in enumerate(kinds):
        size, me = lax.axis_size(axis), lax.axis_index(axis)
        source, result = sources[op], results[op]
        core = lax.rem(me, CORES)
        spot = lax.div(me, CORES)
        partner = me + 1 - 2 * core
        if name == "gather":
            for step in range(1, size):
                copy = remote(op, source, result.at[me], step - 1, axis, lax.rem(me + step, size))
                copy.start()
                simple.append(copy)
            locals_.append(pltpu.make_async_copy(source, result.at[me], local_sem.at[op]))
        elif name == "columns":
            width = result.shape[-1]

            def column(index):
                return source.at[:, pl.ds(pl.multiple_of(index * width, width), width)]

            for step in range(1, size):
                peer = lax.rem(me + step, size)
                copy = remote(op, column(peer), result.at[me], step - 1, axis, peer)
                copy.start()
                simple.append(copy)
            locals_.append(pltpu.make_async_copy(column(me), result.at[me], local_sem.at[op]))
        elif name == "scatter":
            for step in range(1, size):
                peer = lax.rem(me + step, size)
                copy = remote(op, source.at[peer], result.at[me], step - 1, axis, peer)
                copy.start()
                simple.append(copy)
            locals_.append(pltpu.make_async_copy(source.at[me], result.at[me], local_sem.at[op]))
        elif name == "partner":
            for chip in range(size // CORES):
                copy = remote(
                    op, source.at[chip * CORES + 1 - core], result.at[chip], chip, axis, partner
                )
                copy.start()
                simple.append(copy)
        elif name == "stride":
            chips = size // CORES
            for step in range(1, chips):
                other = lax.rem(spot + step, chips)
                copy = remote(
                    op, source.at[other], result.at[spot], step - 1, axis, other * CORES + core
                )
                copy.start()
                simple.append(copy)
            locals_.append(pltpu.make_async_copy(source.at[spot], result.at[spot], local_sem.at[op]))
        else:
            chains.append((op, axis, size // CORES, me, core, spot, partner, source, result))
    for copy in locals_:
        copy.start()

    def hop(chain, source, block, slot, peer):
        op, axis, result = chain[0], chain[1], chain[-1]
        return remote(op, source, result.at[block], slot, axis, peer)

    for chain in chains:
        op, axis, chips, me, core, spot, partner, source, result = chain

        @pl.when(spot + 1 < chips)
        def _():
            hop(chain, source, me, 0, me + CORES).start()

        @pl.when(spot > 0)
        def _():
            hop(chain, source, me, chips - 1, me - CORES).start()

    for chain in chains:
        op, axis, chips, me, core, spot, partner, source, result = chain
        hop(chain, source, me, 2 * (chips - 1), partner).start()
        pltpu.make_async_copy(source, result.at[me], local_sem.at[op]).start()
    for step in range(1, max([chain[2] for chain in chains], default=0)):
        for chain in chains:
            op, axis, chips, me, core, spot, partner, source, result = chain
            for sign, base in ((1, 0), (-1, chips - 1)):
                origin_spot = spot - sign * step
                here = (origin_spot >= 0) & (origin_spot < chips)
                onward = (spot + sign >= 0) & (spot + sign < chips)
                block = me - sign * step * CORES

                @pl.when(here)
                def _():
                    held = result.at[block]
                    hop(chain, held, block, base + step - 1, me).wait_recv()

                    @pl.when(onward)
                    def _():
                        hop(chain, held, block, base + step, me + sign * CORES).start()

                    slot = 2 * (chips - 1) + lax.rem(origin_spot - spot + chips, chips)
                    hop(chain, held, block, slot, partner).start()

    for chain in chains:
        op, axis, chips, me, core, spot, partner, source, result = chain
        for step in range(chips):
            for_spot = lax.rem(spot + step, chips)
            block = for_spot * CORES + core
            theirs = for_spot * CORES + 1 - core
            slot = 2 * (chips - 1) + step
            hop(chain, result.at[block], block, slot, partner).wait_send()
            hop(chain, result.at[theirs], theirs, slot, partner).wait_recv()
        for step in range(chips - 1):
            for sign, base in ((1, 0), (-1, chips - 1)):
                origin_spot = spot - sign * step
                sent = (
                    (origin_spot >= 0)
                    & (origin_spot < chips)
                    & (spot + sign >= 0)
                    & (spot + sign < chips)
                )
                block = me - sign * step * CORES

                @pl.when(sent)
                def _():
                    hop(chain, source, block, base + step, partner).wait_send()

        pltpu.make_async_copy(source, result.at[me], local_sem.at[op]).wait()
    for copy in simple:
        copy.wait()
    for copy in locals_:
        copy.wait()


def exchange(kinds, arrays, number):
    kinds = tuple(kinds)
    shapes = []
    for (name, axis), array in zip(kinds, arrays):
        size = lax.axis_size(axis)
        if name in ("gather", "chain"):
            shape = (size,) + array.shape
        elif name == "columns":
            shape = (size, array.shape[0], array.shape[1] // size)
        elif name == "scatter":
            shape = array.shape
        else:
            shape = (size // CORES,) + array.shape[1:]
        shapes.append(jax.ShapeDtypeStruct(shape, array.dtype))
    sems = [pltpu.SemaphoreType.DMA((count_copies(kind),)) for kind in kinds]
    return pl.pallas_call(
        functools.partial(exchange_kernel, kinds),
        out_shape=shapes,
        in_specs=[pl.BlockSpec(memory_space=pl.ANY)] * len(kinds),
        out_specs=[pl.BlockSpec(memory_space=pl.ANY)] * len(kinds),
        scratch_shapes=[pltpu.SemaphoreType.DMA((len(kinds),))] + sems + sems,
        compiler_params=pltpu.CompilerParams(collective_id=number, has_side_effects=True),
        name="exchange",
    )(*arrays)


def swapped(block, axis, bit):
    count = lax.axis_size(axis)
    route = []
    for low in range(count):
        high = low | 1 << bit
        if high != low and high < count:
            route += [(low, high), (high, low)]
    return lax.ppermute(block, axis, route)


def layer_norm(values, gain):
    center = values - jnp.mean(values, axis=-1, keepdims=True)
    spread = jnp.mean(center * center, axis=-1, keepdims=True)
    return center * lax.rsqrt(spread + 1e-05) * gain


def attend_block(block_queries, keys, values, valid, scale, layout):
    scores = (
        jnp.einsum(
            "thd," + layout + "->htk", block_queries, keys, preferred_element_type=jnp.float32
        )
        * scale
    )
    scores = jnp.where(valid[None, None, :], scores, -1e30)
    top = jnp.max(scores, axis=-1, keepdims=True)
    weights = jnp.exp(scores - top)
    probs = (weights / jnp.sum(weights, axis=-1, keepdims=True)).astype(jnp.bfloat16)
    return jnp.einsum("htk," + layout + "->thd", probs, values, preferred_element_type=jnp.float32)


def local(
    image,
    ln_gain,
    fc1_weight,
    fc2_weight,
    projector_weight,
    kv_weight,
    text,
    q_weight,
    o_weight,
    tile_count,
    text_start,
):
    inputs = image[0].astype(jnp.float32)
    group_count = lax.axis_size("mp")
    normed = layer_norm(inputs, ln_gain).astype(jnp.bfloat16)
    up, down, all_normed = exchange(
        (("chain", "mp"), ("chain", "mp"), ("gather", "dp")), (fc1_weight.T, fc2_weight, normed), 0
    )
    up = up.reshape(-1, up.shape[-1])
    down = down.reshape(-1, down.shape[-1])
    all_normed = all_normed.reshape(-1, all_normed.shape[-1])
    hidden = jax.nn.gelu(
        lax.dot_general(
            all_normed, up, (((1,), (1,)), ((), ())), preferred_element_type=jnp.float32
        ),
        approximate=False,
    ).astype(jnp.bfloat16)
    branch = jnp.dot(hidden, down, preferred_element_type=jnp.float32).astype(jnp.bfloat16)
    branch = branch.reshape((lax.axis_size("dp"),) + inputs.shape)

    kv_count = kv_weight.shape[1]
    devices_per_kv = group_count // kv_count
    kv_columns = kv_count * 2 * HEAD_DIM
    flat_kv = kv_weight.reshape(kv_weight.shape[0], kv_columns)
    row_count = projector_weight.shape[0] // lax.axis_size("dp")
    rows = lax.dynamic_slice_in_dim(
        projector_weight, lax.axis_index("dp") * row_count, row_count, axis=0
    )
    folded = jnp.dot(rows, flat_kv, preferred_element_type=jnp.float32).astype(jnp.bfloat16)
    terms, folded = exchange((("scatter", "dp"), ("columns", "mp")), (branch, folded), 1)
    encoded = (inputs + jnp.sum(terms.astype(jnp.float32), axis=0)).astype(jnp.bfloat16)
    folded = jnp.sum(folded.astype(jnp.float32), axis=0).astype(jnp.bfloat16)
    for bit_index in range(devices_per_kv.bit_length() - 1):
        partner = swapped(folded, "mp", bit_index)
        is_lower = lax.axis_index("mp") // (1 << bit_index) % 2 == 0
        folded = jnp.where(
            is_lower, jnp.concatenate([folded, partner], 1), jnp.concatenate([partner, folded], 1)
        )
    all_encoded, folded = exchange((("chain", "mp"), ("gather", "dp")), (encoded, folded), 2)
    all_encoded = all_encoded.reshape(-1, all_encoded.shape[-1])
    folded = folded.reshape(-1, folded.shape[-1])
    image_rows = all_encoded.shape[0]
    portion = jnp.einsum("rc,kr->ck", folded, all_encoded, preferred_element_type=jnp.float32)
    keys = portion[:HEAD_DIM]
    key_scale = lax.rsqrt(jnp.mean(keys * keys, axis=0, keepdims=True) + 1e-06)
    keys = (keys * key_scale).astype(jnp.bfloat16)
    values = portion[HEAD_DIM:].astype(jnp.bfloat16)
    layout = "dk"
    text_rows = text.shape[1]
    local_heads = q_weight.shape[1] // HEAD_DIM
    queries = jnp.dot(text[0], q_weight, preferred_element_type=jnp.float32).astype(jnp.bfloat16)
    queries = queries.reshape(text_rows, local_heads, HEAD_DIM)
    valid = jnp.arange(image_rows, dtype=jnp.int32) // TILE_TOK < tile_count[0]
    scale = 1.0 / HEAD_DIM**0.5
    block_rows = min(text_rows, 256)
    blocks = queries.reshape(text_rows // block_rows, block_rows, local_heads, HEAD_DIM)
    attended_heads = lax.map(
        lambda block_queries: attend_block(block_queries, keys, values, valid, scale, layout),
        blocks,
    )
    attended_heads = attended_heads.reshape(text_rows, local_heads * HEAD_DIM)
    row_mask = (jnp.arange(text_rows, dtype=jnp.int32) >= text_start[0]).astype(jnp.float32)
    heads_out = (attended_heads * row_mask[:, None]).astype(jnp.bfloat16)
    out = jnp.dot(heads_out, o_weight, preferred_element_type=jnp.float32).astype(jnp.bfloat16)
    out = out.reshape(group_count, text_rows // group_count, out.shape[-1])
    (theirs,) = exchange((("partner", "mp"),), (out,), 3)
    chip_out = out.reshape((group_count // CORES, CORES) + out.shape[1:])
    mine = lax.dynamic_index_in_dim(
        chip_out, lax.axis_index("mp") % CORES, axis=1, keepdims=False
    )
    paired = (mine.astype(jnp.float32) + theirs.astype(jnp.float32)).astype(jnp.bfloat16)
    (terms,) = exchange((("stride", "mp"),), (paired,), 4)
    summed_out = jnp.sum(terms.astype(jnp.float32), axis=0).astype(jnp.bfloat16)
    return summed_out[None]


def erf_gelu(values):
    return 0.5 * values * (1.0 + lax.erf(values * 0.5**0.5))


def fused_kernel(
    image,
    gain,
    fc1,
    fc2,
    projector,
    kv,
    text,
    q_weight,
    o_weight,
    tile_count,
    text_start,
    out,
    up,
    down,
    pixels,
    normed,
    total,
    held,
    x_send,
    x_recv,
    z_send,
    z_recv,
    encoded,
    rows_part,
    kv_raw,
    kv_flat,
    fold_part,
    fold_0,
    fold_1,
    fold_2,
    fold_3,
    fold_4,
    fold_own,
    folded,
    words,
    staged,
    q_total,
    queries,
    keys,
    values,
    mixed,
    tops,
    sums,
    heads,
    o_part,
    o_0,
    o_1,
    o_2,
    o_3,
    o_4,
    local_sem,
    stage_sem,
    sends,
    recvs,
):
    dp, mp = lax.axis_index("dp"), lax.axis_index("mp")
    core, spot = lax.rem(mp, CORES), lax.div(mp, CORES)
    low, high = lax.rem(spot, 2), lax.div(spot, 2)
    spot_1 = spot + 1 - 2 * low
    spot_2 = spot + 2 - 4 * high
    spot_3 = spot_1 + 2 - 4 * high
    dp_x = dp + 1 - 2 * lax.rem(dp, 2)
    dp_y = dp + 2 - 4 * lax.div(dp, 2)
    pc = {"mp": spot * CORES + 1 - core}
    x1, y1 = {"dp": dp_x}, {"dp": dp_y}
    z1 = {"mp": spot_1 * CORES + core}
    z2 = {"mp": spot_2 * CORES + core}

    barrier = pltpu.get_barrier_semaphore()
    for peer in (pc, x1, y1, z1, z2):
        pl.semaphore_signal(barrier, inc=1, device_id=peer, device_id_type=MESH)

    locals_ = []

    def local(source, target):
        copy = pltpu.make_async_copy(source, target, local_sem.at[len(locals_)])
        copy.start()
        locals_.append(copy)
        return copy

    rows = image.shape[0]
    hidden = fc1.shape[0]
    part_rows = rows_part.shape[0]
    depth = staged.shape[1]
    stages = staged.shape[0]

    def q_copy(step):
        slot = lax.rem(step, stages)
        return pltpu.make_async_copy(
            q_weight.at[pl.ds(pl.multiple_of(step * depth, depth), depth)],
            staged.at[slot],
            stage_sem.at[slot],
        )

    def o_copy(step):
        slot = lax.rem(step, stages)
        return pltpu.make_async_copy(
            o_weight.at[:, pl.ds(pl.multiple_of(step * depth, depth), depth)],
            staged.at[slot],
            stage_sem.at[slot],
        )

    image_copy = local(image, pixels.at[0])
    up_copy = local(fc1, up.at[0, pl.ds(0, hidden)])
    down_copy = local(fc2, down.at[0, pl.ds(0, hidden)])
    text_copy = local(text, words)
    for step in range(stages):
        q_copy(step).start()
    kv_copy = local(kv, kv_raw)
    part_copy = local(
        projector.at[pl.ds(pl.multiple_of(dp * part_rows, part_rows), part_rows)], rows_part
    )

    pl.semaphore_wait(barrier, 5)

    started = []

    def remote(source, target, peer):
        slot = len(started)
        copy = pltpu.make_async_remote_copy(
            src_ref=source,
            dst_ref=target,
            send_sem=sends.at[slot],
            recv_sem=recvs.at[slot],
            device_id=peer,
            device_id_type=MESH,
        )
        copy.start()
        started.append(copy)
        return copy

    mine, theirs = pl.ds(0, hidden), pl.ds(hidden, hidden)
    parts = x_send.shape[1]
    slim = rows // parts
    slices = [pl.ds(part * slim, slim) for part in range(parts)]
    piece = 32
    bits = [pl.ds(begin, piece) for begin in range(0, hidden, piece)]
    image_z = [remote(image.at[area], pixels.at[2, area], z1) for area in slices]
    image_x = remote(image, pixels.at[1], x1)
    up_z = [remote(fc1.at[area], up.at[2, area], z2) for area in bits]
    down_z = [remote(fc2.at[area], down.at[2, area], z2) for area in bits]
    up_y = remote(fc1, up.at[1, mine], y1)
    down_y = remote(fc2, down.at[1, mine], y1)
    up_p = {0: remote(fc1, up.at[0, theirs], pc)}
    down_p = {0: remote(fc2, down.at[0, theirs], pc)}

    text_copy.wait()
    q_steps = q_weight.shape[0] // depth
    q_total[...] = jnp.zeros_like(q_total)

    def q_step(step, carry):
        q_copy(step).wait()
        q_total[...] += jnp.dot(
            words[:, pl.ds(pl.multiple_of(step * depth, depth), depth)],
            staged[lax.rem(step, stages)],
            preferred_element_type=jnp.float32,
        )

        @pl.when(step + stages < q_steps)
        def _():
            q_copy(step + stages).start()

        return carry

    lax.fori_loop(0, q_steps, q_step, 0)
    text_rows = words.shape[0]
    head_count = q_total.shape[1] // HEAD_DIM
    for head in range(head_count):
        queries[head // 2, pl.ds(head % 2 * text_rows, text_rows)] = q_total[
            :, head * HEAD_DIM : (head + 1) * HEAD_DIM
        ].astype(jnp.bfloat16)

    strip = 32

    def normalise(block):
        def one(step, carry):
            spot_rows = pl.ds(pl.multiple_of(step * strip, strip), strip)
            entry = pixels[block, spot_rows].astype(jnp.float32)
            normed[block, spot_rows] = layer_norm(entry, gain[...]).astype(jnp.bfloat16)
            return carry

        lax.fori_loop(0, rows // strip, one, 0)

    tile = 256

    def mlp(block, first, last, base, stride=1):
        def one(step, carry):
            row = base + step * stride
            inner = lax.dot_general(
                normed[row], up[block], (((1,), (1,)), ((), ())), preferred_element_type=jnp.float32
            )
            inner = erf_gelu(inner).astype(jnp.bfloat16)
            for begin in range(0, total.shape[-1], tile):
                area = pl.ds(begin, tile)
                term = jnp.dot(inner, down[block, :, area], preferred_element_type=jnp.float32)
                if first:
                    total[row, :, area] = term
                else:
                    total[row, :, area] += term
            return carry

        lax.fori_loop(0, last, one, 0)

    def widen(block, last, base, stride=1):
        def one(step, carry):
            row = base + step * stride
            inner = lax.dot_general(
                normed[row], up[block], (((1,), (1,)), ((), ())), preferred_element_type=jnp.float32
            )
            held[block - 2, row] = erf_gelu(inner).astype(jnp.bfloat16)
            return carry

        lax.fori_loop(0, last, one, 0)

    def narrow(block, last, base, stride=1):
        def one(step, carry):
            row = base + step * stride
            for begin in range(0, total.shape[-1], tile):
                area = pl.ds(begin, tile)
                total[row, :, area] += jnp.dot(
                    held[block - 2, row], down[block, :, area], preferred_element_type=jnp.float32
                )
            return carry

        lax.fori_loop(0, last, one, 0)

    image_copy.wait()
    up_copy.wait()
    down_copy.wait()
    normalise(0)
    up_p[0].wait_recv()
    down_p[0].wait_recv()
    mlp(0, True, 1, 0)
    kv_copy.wait()
    flat = 16

    def flatten(step, carry):
        area = pl.ds(pl.multiple_of(step * flat, flat), flat)
        kv_flat[area] = kv_raw[area].reshape(flat, kv_flat.shape[1])
        return carry

    lax.fori_loop(0, kv_flat.shape[0] // flat, flatten, 0)
    part_copy.wait()
    columns = fold_part.shape[-1]

    def fold_step(head, carry):
        block = kv_flat[:, pl.ds(pl.multiple_of(head * columns, columns), columns)]
        fold_part[lax.div(head, CORES), lax.rem(head, CORES)] = jnp.dot(
            rows_part[...], block, preferred_element_type=jnp.float32
        ).astype(jnp.bfloat16)
        return carry

    lax.fori_loop(0, fold_part.shape[0] * CORES, fold_step, 0)
    fold_p = remote(fold_part.at[:, 1 - core], fold_0, pc)
    for step in range(stages):
        o_copy(step).start()
    image_x.wait_recv()
    normalise(1)
    mlp(0, True, 1, 1)
    up_y.wait_recv()
    up_p[1] = remote(up.at[1, mine], up.at[1, theirs], pc)
    down_y.wait_recv()
    down_p[1] = remote(down.at[1, mine], down.at[1, theirs], pc)
    up_d, down_d = [], []
    for part, copy in enumerate(up_z):
        copy.wait_recv()
        up_d.append(remote(up.at[2, bits[part]], up.at[3, bits[part]], y1))
    up_p[2] = remote(up.at[2, mine], up.at[2, theirs], pc)
    image_d = []

    def image_on(part):
        image_z[part].wait_recv()
        image_d.append(remote(pixels.at[2, slices[part]], pixels.at[3, slices[part]], x1))

    def down_on(part):
        down_z[part].wait_recv()
        down_d.append(remote(down.at[2, bits[part]], down.at[3, bits[part]], y1))

    for part in range(parts - 1):
        image_on(part)
    up_p[1].wait_recv()
    down_p[1].wait_recv()
    mlp(1, False, 2, 0)
    down_on(0)
    up_p[2].wait_recv()
    widen(2, 2, 0)
    image_on(parts - 1)
    down_on(1)
    normalise(2)
    down_on(2)
    mlp(0, True, 1, 2)
    mlp(1, False, 1, 2)
    for part in range(3, len(bits)):
        down_on(part)
    down_p[2] = remote(down.at[2, mine], down.at[2, theirs], pc)
    fold_p.wait_recv()
    spots = fold_0.shape[0]

    def fold_pair(index, carry):
        fold_1[lax.div(index, 2), lax.rem(index, 2)] = (
            fold_part[index, core].astype(jnp.float32) + fold_0[index].astype(jnp.float32)
        ).astype(jnp.bfloat16)
        return carry

    lax.fori_loop(0, spots, fold_pair, 0)
    fold_z = remote(fold_1.at[:, 1 - low], fold_2, z1)
    for copy in up_d:
        copy.wait_recv()
    up_p[3] = remote(up.at[3, mine], up.at[3, theirs], pc)
    up_p[3].wait_recv()
    widen(3, 1, 1)
    down_p[2].wait_recv()
    narrow(2, 1, 1)
    for copy in image_d:
        copy.wait_recv()
    normalise(3)
    mlp(0, True, 1, 3)
    mlp(1, False, 1, 3)
    widen(2, 1, 3)
    spread = []
    for part, copy in enumerate(down_d):
        copy.wait_recv()
        mirror = pl.ds(hidden + part * piece, piece)
        spread.append(remote(down.at[3, bits[part]], down.at[3, mirror], pc))
    for copy in spread:
        copy.wait_recv()

    def to_x(row, part):
        index = row // 2
        x_send[index, part] = total[row, slices[part]].astype(jnp.bfloat16)
        return remote(x_send.at[index, part], x_recv.at[index, part], x1)

    narrow(3, 1, 1)
    x_copies = {(0, 0): to_x(1, 0), (0, 1): to_x(1, 1)}
    widen(3, 1, 3)
    narrow(2, 1, 3)
    narrow(3, 1, 3)
    order = [(0, 0), (0, 1)]
    for part in range(2, parts):
        order += [(1, part - 2), (0, part)]
    order += [(1, part) for part in range(parts - 2, parts)]
    for index, part in order[2:]:
        x_copies[index, part] = to_x(2 * index + 1, part)
    widen(2, 1, 2)
    widen(3, 2, 0, 2)
    narrow(2, 2, 0, 2)
    narrow(3, 2, 0, 2)
    fold_z.wait_recv()
    for index in range(2):
        fold_3[index] = (
            fold_1[index, low].astype(jnp.float32) + fold_2[index].astype(jnp.float32)
        ).astype(jnp.bfloat16)
    fold_zz = remote(fold_3.at[1 - high], fold_4, z2)

    def fold_rows(owner):
        return folded.at[pl.ds(pl.multiple_of(owner * part_rows, part_rows), part_rows)]

    z_copies, pairs, onward = {}, {}, {}

    def area_of(core_side, part):
        return pl.ds(core_side * rows + part * slim, slim)

    def to_partner(unit, part):
        pairs[unit, part] = remote(
            encoded.at[unit, area_of(0, part)], encoded.at[unit, area_of(1, part)], pc
        )

    def encode(index, part):
        z_copies[1 - index, part].wait_recv()
        area = slices[part]
        encoded[index, area_of(0, part)] = (
            pixels[2 * index, area].astype(jnp.float32)
            + total[2 * index, area]
            + z_recv[index, part].astype(jnp.float32)
        ).astype(jnp.bfloat16)
        if index == 0:
            onward[2, part] = remote(
                encoded.at[0, area_of(0, part)], encoded.at[2, area_of(0, part)], z2
            )
        to_partner(index, part)

    ready = [(index, part) for part in range(parts) for index in range(2)]
    count = 0
    for number, (index, part) in enumerate(order):
        x_copies[index, part].wait_recv()
        area = slices[part]
        met = total[2 * index, area] + x_recv[index, part].astype(jnp.float32)
        total[2 * index, area] = met
        z_send[index, part] = met.astype(jnp.bfloat16)
        z_copies[index, part] = remote(z_send.at[index, part], z_recv.at[1 - index, part], z1)
        if number == 1:
            fold_zz.wait_recv()
            fold_own[...] = (
                fold_3[high].astype(jnp.float32) + fold_4[...].astype(jnp.float32)
            ).astype(jnp.bfloat16)
            fold_local = local(fold_own, fold_rows(dp))
            fold_y = remote(fold_own, fold_rows(dp), y1)
            fold_x = remote(fold_own, fold_rows(dp), x1)
        if number in (5, 7):
            encode(*ready[count])
            encode(*ready[count + 1])
            count += 2
    for entry in ready[count:]:
        encode(*entry)

    fold_x.wait_recv()
    fold_d = remote(fold_rows(dp_x), fold_rows(dp_x), y1)

    def pass_on(part):
        onward[2, part].wait_recv()
        onward[3, part] = remote(
            encoded.at[2, area_of(0, part)], encoded.at[3, area_of(0, part)], z1
        )
        to_partner(2, part)

    def gather(unit):
        for part in range(parts):
            pairs[unit, part].wait_recv()

    pass_on(0)
    pass_on(1)
    pass_on(2)
    fold_local.wait()
    fold_y.wait_recv()
    fold_d.wait_recv()
    scale = 1.0 / HEAD_DIM**0.5
    limit = tile_count[0] * TILE_TOK

    def attend(unit, unit_spot):
        count = 2 * rows
        kv_block = jnp.dot(encoded[unit], folded[...], preferred_element_type=jnp.float32)
        key = kv_block[:, :HEAD_DIM]
        key_scale = lax.rsqrt(jnp.mean(key * key, axis=-1, keepdims=True) + 1e-06)
        keys[...] = (key * key_scale).astype(jnp.bfloat16)
        values[...] = kv_block[:, HEAD_DIM:].astype(jnp.bfloat16)
        place = lax.broadcasted_iota(jnp.int32, (1, count), 1)
        own_base = (unit_spot * CORES + core) * rows
        other_base = (unit_spot * CORES + 1 - core) * rows - rows
        token = place + jnp.where(place < rows, own_base, other_base)
        valid = token < limit

        def one(group, carry):
            scores = (
                lax.dot_general(
                    queries[group],
                    keys[...],
                    (((1,), (1,)), ((), ())),
                    preferred_element_type=jnp.float32,
                )
                * scale
            )
            scores = jnp.where(valid, scores, -1e30)
            top = jnp.max(scores, axis=-1, keepdims=True)
            if unit > 0:
                before = tops[group][:, :1]
                top = jnp.maximum(before, top)
                shrink = jnp.exp(before - top)
            weights = jnp.exp(scores - top)
            weight_sum = jnp.sum(weights, axis=-1, keepdims=True)
            blend = jnp.dot(
                weights.astype(jnp.bfloat16), values[...], preferred_element_type=jnp.float32
            )
            if unit > 0:
                weight_sum += shrink * sums[group][:, :1]
                blend += shrink * mixed[group]
            tops[group] = jnp.broadcast_to(top, tops.shape[1:])
            sums[group] = jnp.broadcast_to(weight_sum, sums.shape[1:])
            mixed[group] = blend
            return carry

        lax.fori_loop(0, queries.shape[0], one, 0)

    gather(0)
    attend(0, spot)
    pass_on(3)
    gather(1)
    attend(1, spot_1)
    gather(2)
    attend(2, spot_2)
    for part in range(parts):
        onward[3, part].wait_recv()
        to_partner(3, part)
    gather(3)
    attend(3, spot_3)

    text_at = lax.broadcasted_iota(jnp.int32, (text_rows, 1), 0)
    row_mask = (text_at >= text_start[0]).astype(jnp.float32)
    for head in range(head_count):
        area = pl.ds(head % 2 * text_rows, text_rows)
        heads[:, head * HEAD_DIM : (head + 1) * HEAD_DIM] = (
            mixed[head // 2, area] / sums[head // 2, area][:, :1] * row_mask
        ).astype(jnp.bfloat16)

    steps = o_part.shape[0]
    base = len(started)

    def o_remote(kind, step, source, target, peer):
        return pltpu.make_async_remote_copy(
            src_ref=source,
            dst_ref=target,
            send_sem=sends.at[base + kind * steps + step],
            recv_sem=recvs.at[base + kind * steps + step],
            device_id=peer,
            device_id_type=MESH,
        )

    def o_first(step):
        return o_remote(0, step, o_part.at[step, :, :, 1 - core], o_0.at[step], pc)

    def o_second(step):
        return o_remote(1, step, o_1.at[step, :, 1 - low], o_2.at[step], z1)

    def o_third(step):
        return o_remote(2, step, o_3.at[step, 1 - high], o_4.at[step], z2)

    def meet_first(step):
        o_first(step).wait_recv()
        o_1[step] = (
            o_part[step, :, :, core].astype(jnp.float32) + o_0[step].astype(jnp.float32)
        ).astype(jnp.bfloat16)
        o_second(step).start()

    def meet_second(step):
        o_second(step).wait_recv()
        o_3[step] = (
            o_1[step, :, low].astype(jnp.float32) + o_2[step].astype(jnp.float32)
        ).astype(jnp.bfloat16)
        o_third(step).start()

    def o_step(step, carry):
        o_copy(step).wait()
        slot = lax.rem(step, stages)
        result = jnp.dot(heads[...], staged[slot], preferred_element_type=jnp.float32)
        o_part[step] = result.reshape(o_part.shape[1:]).astype(jnp.bfloat16)
        o_first(step).start()

        @pl.when(step + stages < steps)
        def _():
            o_copy(step + stages).start()

        @pl.when(step > 1)
        def _():
            meet_first(step - 2)

        return carry

    lax.fori_loop(0, steps, o_step, 0)
    meet_first(steps - 2)
    meet_first(steps - 1)

    def second(step, carry):
        meet_second(step)
        return carry

    lax.fori_loop(0, steps, second, 0)

    def third(step, carry):
        o_third(step).wait_recv()
        out[:, pl.ds(pl.multiple_of(step * depth, depth), depth)] = (
            o_3[step, high].astype(jnp.float32) + o_4[step].astype(jnp.float32)
        ).astype(jnp.bfloat16)
        return carry

    lax.fori_loop(0, steps, third, 0)
    for copy in started:
        copy.wait_send()

    def drain(step, carry):
        o_first(step).wait_send()
        o_second(step).wait_send()
        o_third(step).wait_send()
        return carry

    lax.fori_loop(0, steps, drain, 0)


def fused(image, gain, fc1, fc2, projector, kv, text, q_weight, o_weight, tile_count, text_start):
    rows, width = image.shape
    hidden = fc1.shape[0]
    part_rows = projector.shape[0] // lax.axis_size("dp")
    depth = projector.shape[1]
    kv_columns = kv.shape[1] * kv.shape[2] * kv.shape[3]
    columns = kv_columns // lax.axis_size("mp")
    text_rows = text.shape[0]
    query_columns = q_weight.shape[1]
    pairs = query_columns // HEAD_DIM // 2
    parts = 4
    token_rows = text_rows // lax.axis_size("mp")
    steps = o_weight.shape[1] // depth
    low, wide = jnp.bfloat16, jnp.float32
    copies = 96 + 3 * steps
    scratch = [
        ((4, 2 * hidden, width), low),
        ((4, 2 * hidden, width), low),
        ((4, rows, width), low),
        ((4, rows, width), low),
        ((4, rows, width), wide),
        ((2, 4, rows, 2 * hidden), low),
        ((2, parts, rows // parts, width), low),
        ((2, parts, rows // parts, width), low),
        ((2, parts, rows // parts, width), low),
        ((2, parts, rows // parts, width), low),
        ((4, 2 * rows, width), low),
        ((part_rows, depth), low),
        (kv.shape, low),
        ((kv.shape[0], kv_columns), low),
        ((4, CORES, part_rows, columns), low),
        ((4, part_rows, columns), low),
        ((2, 2, part_rows, columns), low),
        ((2, part_rows, columns), low),
        ((2, part_rows, columns), low),
        ((part_rows, columns), low),
        ((part_rows, columns), low),
        ((width, columns), low),
        (text.shape, low),
        ((4, depth, depth), low),
        ((text_rows, query_columns), wide),
        ((pairs, 2 * text_rows, HEAD_DIM), low),
        ((2 * rows, HEAD_DIM), low),
        ((2 * rows, HEAD_DIM), low),
        ((pairs, 2 * text_rows, HEAD_DIM), wide),
        ((pairs, 2 * text_rows, HEAD_DIM), wide),
        ((pairs, 2 * text_rows, HEAD_DIM), wide),
        ((text_rows, query_columns), low),
        ((steps, 2, 2, CORES, token_rows, depth), low),
        ((steps, 2, 2, token_rows, depth), low),
        ((steps, 2, 2, token_rows, depth), low),
        ((steps, 2, token_rows, depth), low),
        ((steps, 2, token_rows, depth), low),
        ((steps, token_rows, depth), low),
    ]
    vmem, anywhere = pl.BlockSpec(memory_space=pltpu.VMEM), pl.BlockSpec(memory_space=pl.ANY)
    smem = pl.BlockSpec(memory_space=pltpu.SMEM)
    return pl.pallas_call(
        fused_kernel,
        out_shape=jax.ShapeDtypeStruct((token_rows, o_weight.shape[1]), jnp.bfloat16),
        in_specs=[anywhere, vmem] + [anywhere] * 7 + [smem, smem],
        out_specs=vmem,
        scratch_shapes=[pltpu.VMEM(shape, kind) for shape, kind in scratch]
        + [
            pltpu.SemaphoreType.DMA((16,)),
            pltpu.SemaphoreType.DMA((4,)),
            pltpu.SemaphoreType.DMA((copies,)),
            pltpu.SemaphoreType.DMA((copies,)),
        ],
        compiler_params=pltpu.CompilerParams(
            collective_id=7, has_side_effects=True, vmem_limit_bytes=67043328
        ),
        name="fused",
    )(image, gain, fc1, fc2, projector, kv, text, q_weight, o_weight, tile_count, text_start)


def paired_local(
    image,
    ln_gain,
    fc1_weight,
    fc2_weight,
    projector_weight,
    kv_weight,
    text,
    q_weight,
    o_weight,
    tile_count,
    text_start,
):
    return fused(
        image[0],
        ln_gain,
        fc1_weight.T,
        fc2_weight,
        projector_weight,
        kv_weight,
        text[0],
        q_weight,
        o_weight,
        tile_count,
        text_start,
    )[None]


def choose(*arrays):
    groups, members = lax.axis_size("dp"), lax.axis_size("mp")
    pairs_of_pairs = groups == members // CORES == 2 * 2
    if pairs_of_pairs and arrays[5].shape[1] == members:
        return paired_local(*arrays)
    return local(*arrays)


def solution(mesh):
    return jax.shard_map(
        choose,
        mesh=mesh,
        in_specs=(
            P("dp", "mp", None),
            P(),
            P(None, ("dp", "mp")),
            P(("dp", "mp"), None),
            P(None, "mp"),
            P("mp", None, None, None),
            P("dp", None, None),
            P(None, "mp"),
            P("mp", None),
            P("dp"),
            P("dp"),
        ),
        out_specs=P("dp", "mp", None),
        check_vma=False,
    )
```

```python
import functools

import jax
import jax.numpy as jnp
from jax import lax
from jax.experimental import pallas as pl
from jax.experimental.pallas import tpu as pltpu
from jax.sharding import PartitionSpec as P

HEAD_DIM = 128
TILE_TOK = 512

MESH = pl.DeviceIdType.MESH
CORES = 2


def count_copies(kind):
    name, axis = kind
    size = lax.axis_size(axis)
    if name == "chain":
        return 2 * (size // CORES - 1) + size // CORES
    if name == "partner":
        return size // CORES
    if name == "stride":
        return size // CORES - 1
    return size - 1


def exchange_kernel(kinds, *refs):
    count = len(kinds)
    sources, results = refs[:count], refs[count : 2 * count]
    local_sem = refs[2 * count]
    sends, recvs = refs[2 * count + 1 : 3 * count + 1], refs[3 * count + 1 :]
    axes = sorted({axis for _, axis in kinds})

    barrier = pltpu.get_barrier_semaphore()
    greeted = 0
    for axis in axes:
        size, me = lax.axis_size(axis), lax.axis_index(axis)
        for step in range(1, size):
            pl.semaphore_signal(
                barrier, inc=1, device_id={axis: lax.rem(me + step, size)}, device_id_type=MESH
            )
        greeted += size - 1
    pl.semaphore_wait(barrier, greeted)

    def remote(op, source, result, slot, axis, peer):
        return pltpu.make_async_remote_copy(
            src_ref=source,
            dst_ref=result,
            send_sem=sends[op].at[slot],
            recv_sem=recvs[op].at[slot],
            device_id={axis: peer},
            device_id_type=MESH,
        )

    simple, chains, locals_ = [], [], []
    for op, (name, axis) in enumerate(kinds):
        size, me = lax.axis_size(axis), lax.axis_index(axis)
        source, result = sources[op], results[op]
        core = lax.rem(me, CORES)
        spot = lax.div(me, CORES)
        partner = me + 1 - 2 * core
        if name == "gather":
            for step in range(1, size):
                copy = remote(op, source, result.at[me], step - 1, axis, lax.rem(me + step, size))
                copy.start()
                simple.append(copy)
            locals_.append(pltpu.make_async_copy(source, result.at[me], local_sem.at[op]))
        elif name == "columns":
            width = result.shape[-1]

            def column(index):
                return source.at[:, pl.ds(pl.multiple_of(index * width, width), width)]

            for step in range(1, size):
                peer = lax.rem(me + step, size)
                copy = remote(op, column(peer), result.at[me], step - 1, axis, peer)
                copy.start()
                simple.append(copy)
            locals_.append(pltpu.make_async_copy(column(me), result.at[me], local_sem.at[op]))
        elif name == "scatter":
            for step in range(1, size):
                peer = lax.rem(me + step, size)
                copy = remote(op, source.at[peer], result.at[me], step - 1, axis, peer)
                copy.start()
                simple.append(copy)
            locals_.append(pltpu.make_async_copy(source.at[me], result.at[me], local_sem.at[op]))
        elif name == "partner":
            for chip in range(size // CORES):
                copy = remote(
                    op, source.at[chip * CORES + 1 - core], result.at[chip], chip, axis, partner
                )
                copy.start()
                simple.append(copy)
        elif name == "stride":
            chips = size // CORES
            for step in range(1, chips):
                other = lax.rem(spot + step, chips)
                copy = remote(
                    op, source.at[other], result.at[spot], step - 1, axis, other * CORES + core
                )
                copy.start()
                simple.append(copy)
            locals_.append(pltpu.make_async_copy(source.at[spot], result.at[spot], local_sem.at[op]))
        else:
            chains.append((op, axis, size // CORES, me, core, spot, partner, source, result))
    for copy in locals_:
        copy.start()

    def hop(chain, source, block, slot, peer):
        op, axis, result = chain[0], chain[1], chain[-1]
        return remote(op, source, result.at[block], slot, axis, peer)

    for chain in chains:
        op, axis, chips, me, core, spot, partner, source, result = chain

        @pl.when(spot + 1 < chips)
        def _():
            hop(chain, source, me, 0, me + CORES).start()

        @pl.when(spot > 0)
        def _():
            hop(chain, source, me, chips - 1, me - CORES).start()

    for chain in chains:
        op, axis, chips, me, core, spot, partner, source, result = chain
        hop(chain, source, me, 2 * (chips - 1), partner).start()
        pltpu.make_async_copy(source, result.at[me], local_sem.at[op]).start()
    for step in range(1, max([chain[2] for chain in chains], default=0)):
        for chain in chains:
            op, axis, chips, me, core, spot, partner, source, result = chain
            for sign, base in ((1, 0), (-1, chips - 1)):
                origin_spot = spot - sign * step
                here = (origin_spot >= 0) & (origin_spot < chips)
                onward = (spot + sign >= 0) & (spot + sign < chips)
                block = me - sign * step * CORES

                @pl.when(here)
                def _():
                    held = result.at[block]
                    hop(chain, held, block, base + step - 1, me).wait_recv()

                    @pl.when(onward)
                    def _():
                        hop(chain, held, block, base + step, me + sign * CORES).start()

                    slot = 2 * (chips - 1) + lax.rem(origin_spot - spot + chips, chips)
                    hop(chain, held, block, slot, partner).start()

    for chain in chains:
        op, axis, chips, me, core, spot, partner, source, result = chain
        for step in range(chips):
            for_spot = lax.rem(spot + step, chips)
            block = for_spot * CORES + core
            theirs = for_spot * CORES + 1 - core
            slot = 2 * (chips - 1) + step
            hop(chain, result.at[block], block, slot, partner).wait_send()
            hop(chain, result.at[theirs], theirs, slot, partner).wait_recv()
        for step in range(chips - 1):
            for sign, base in ((1, 0), (-1, chips - 1)):
                origin_spot = spot - sign * step
                sent = (
                    (origin_spot >= 0)
                    & (origin_spot < chips)
                    & (spot + sign >= 0)
                    & (spot + sign < chips)
                )
                block = me - sign * step * CORES

                @pl.when(sent)
                def _():
                    hop(chain, source, block, base + step, partner).wait_send()

        pltpu.make_async_copy(source, result.at[me], local_sem.at[op]).wait()
    for copy in simple:
        copy.wait()
    for copy in locals_:
        copy.wait()


def exchange(kinds, arrays, number):
    kinds = tuple(kinds)
    shapes = []
    for (name, axis), array in zip(kinds, arrays):
        size = lax.axis_size(axis)
        if name in ("gather", "chain"):
            shape = (size,) + array.shape
        elif name == "columns":
            shape = (size, array.shape[0], array.shape[1] // size)
        elif name == "scatter":
            shape = array.shape
        else:
            shape = (size // CORES,) + array.shape[1:]
        shapes.append(jax.ShapeDtypeStruct(shape, array.dtype))
    sems = [pltpu.SemaphoreType.DMA((count_copies(kind),)) for kind in kinds]
    return pl.pallas_call(
        functools.partial(exchange_kernel, kinds),
        out_shape=shapes,
        in_specs=[pl.BlockSpec(memory_space=pl.ANY)] * len(kinds),
        out_specs=[pl.BlockSpec(memory_space=pl.ANY)] * len(kinds),
        scratch_shapes=[pltpu.SemaphoreType.DMA((len(kinds),))] + sems + sems,
        compiler_params=pltpu.CompilerParams(collective_id=number, has_side_effects=True),
        name="exchange",
    )(*arrays)


def swapped(block, axis, bit):
    count = lax.axis_size(axis)
    route = []
    for low in range(count):
        high = low | 1 << bit
        if high != low and high < count:
            route += [(low, high), (high, low)]
    return lax.ppermute(block, axis, route)


def layer_norm(values, gain):
    center = values - jnp.mean(values, axis=-1, keepdims=True)
    spread = jnp.mean(center * center, axis=-1, keepdims=True)
    return center * lax.rsqrt(spread + 1e-05) * gain


def attend_block(block_queries, keys, values, valid, scale, layout):
    scores = (
        jnp.einsum(
            "thd," + layout + "->htk", block_queries, keys, preferred_element_type=jnp.float32
        )
        * scale
    )
    scores = jnp.where(valid[None, None, :], scores, -1e30)
    top = jnp.max(scores, axis=-1, keepdims=True)
    weights = jnp.exp(scores - top)
    probs = (weights / jnp.sum(weights, axis=-1, keepdims=True)).astype(jnp.bfloat16)
    return jnp.einsum("htk," + layout + "->thd", probs, values, preferred_element_type=jnp.float32)


def local(
    image,
    ln_gain,
    fc1_weight,
    fc2_weight,
    projector_weight,
    kv_weight,
    text,
    q_weight,
    o_weight,
    tile_count,
    text_start,
):
    inputs = image[0].astype(jnp.float32)
    group_count = lax.axis_size("mp")
    normed = layer_norm(inputs, ln_gain).astype(jnp.bfloat16)
    up, down, all_normed = exchange(
        (("chain", "mp"), ("chain", "mp"), ("gather", "dp")), (fc1_weight.T, fc2_weight, normed), 0
    )
    up = up.reshape(-1, up.shape[-1])
    down = down.reshape(-1, down.shape[-1])
    all_normed = all_normed.reshape(-1, all_normed.shape[-1])
    hidden = jax.nn.gelu(
        lax.dot_general(
            all_normed, up, (((1,), (1,)), ((), ())), preferred_element_type=jnp.float32
        ),
        approximate=False,
    ).astype(jnp.bfloat16)
    branch = jnp.dot(hidden, down, preferred_element_type=jnp.float32).astype(jnp.bfloat16)
    branch = branch.reshape((lax.axis_size("dp"),) + inputs.shape)

    kv_count = kv_weight.shape[1]
    devices_per_kv = group_count // kv_count
    kv_columns = kv_count * 2 * HEAD_DIM
    flat_kv = kv_weight.reshape(kv_weight.shape[0], kv_columns)
    row_count = projector_weight.shape[0] // lax.axis_size("dp")
    rows = lax.dynamic_slice_in_dim(
        projector_weight, lax.axis_index("dp") * row_count, row_count, axis=0
    )
    folded = jnp.dot(rows, flat_kv, preferred_element_type=jnp.float32).astype(jnp.bfloat16)
    terms, folded = exchange((("scatter", "dp"), ("columns", "mp")), (branch, folded), 1)
    encoded = (inputs + jnp.sum(terms.astype(jnp.float32), axis=0)).astype(jnp.bfloat16)
    folded = jnp.sum(folded.astype(jnp.float32), axis=0).astype(jnp.bfloat16)
    for bit_index in range(devices_per_kv.bit_length() - 1):
        partner = swapped(folded, "mp", bit_index)
        is_lower = lax.axis_index("mp") // (1 << bit_index) % 2 == 0
        folded = jnp.where(
            is_lower, jnp.concatenate([folded, partner], 1), jnp.concatenate([partner, folded], 1)
        )
    all_encoded, folded = exchange((("chain", "mp"), ("gather", "dp")), (encoded, folded), 2)
    all_encoded = all_encoded.reshape(-1, all_encoded.shape[-1])
    folded = folded.reshape(-1, folded.shape[-1])
    image_rows = all_encoded.shape[0]
    portion = jnp.einsum("rc,kr->ck", folded, all_encoded, preferred_element_type=jnp.float32)
    keys = portion[:HEAD_DIM]
    key_scale = lax.rsqrt(jnp.mean(keys * keys, axis=0, keepdims=True) + 1e-06)
    keys = (keys * key_scale).astype(jnp.bfloat16)
    values = portion[HEAD_DIM:].astype(jnp.bfloat16)
    layout = "dk"
    text_rows = text.shape[1]
    local_heads = q_weight.shape[1] // HEAD_DIM
    queries = jnp.dot(text[0], q_weight, preferred_element_type=jnp.float32).astype(jnp.bfloat16)
    queries = queries.reshape(text_rows, local_heads, HEAD_DIM)
    valid = jnp.arange(image_rows, dtype=jnp.int32) // TILE_TOK < tile_count[0]
    scale = 1.0 / HEAD_DIM**0.5
    block_rows = min(text_rows, 256)
    blocks = queries.reshape(text_rows // block_rows, block_rows, local_heads, HEAD_DIM)
    attended_heads = lax.map(
        lambda block_queries: attend_block(block_queries, keys, values, valid, scale, layout),
        blocks,
    )
    attended_heads = attended_heads.reshape(text_rows, local_heads * HEAD_DIM)
    row_mask = (jnp.arange(text_rows, dtype=jnp.int32) >= text_start[0]).astype(jnp.float32)
    heads_out = (attended_heads * row_mask[:, None]).astype(jnp.bfloat16)
    out = jnp.dot(heads_out, o_weight, preferred_element_type=jnp.float32).astype(jnp.bfloat16)
    out = out.reshape(group_count, text_rows // group_count, out.shape[-1])
    (theirs,) = exchange((("partner", "mp"),), (out,), 3)
    chip_out = out.reshape((group_count // CORES, CORES) + out.shape[1:])
    mine = lax.dynamic_index_in_dim(
        chip_out, lax.axis_index("mp") % CORES, axis=1, keepdims=False
    )
    paired = (mine.astype(jnp.float32) + theirs.astype(jnp.float32)).astype(jnp.bfloat16)
    (terms,) = exchange((("stride", "mp"),), (paired,), 4)
    summed_out = jnp.sum(terms.astype(jnp.float32), axis=0).astype(jnp.bfloat16)
    return summed_out[None]


def erf_gelu(values):
    return 0.5 * values * (1.0 + lax.erf(values * 0.5**0.5))


def fused_kernel(
    image,
    gain_from,
    fc1,
    fc2,
    projector,
    kv,
    text,
    q_weight,
    o_weight,
    tiles_from,
    start_from,
    out,
    up,
    down,
    pixels,
    normed,
    total,
    held,
    x_send,
    x_recv,
    z_send,
    z_recv,
    encoded,
    rows_part,
    kv_raw,
    kv_flat,
    fold_part,
    fold_0,
    fold_1,
    fold_2,
    fold_3,
    fold_4,
    fold_own,
    folded,
    words,
    staged,
    q_total,
    queries,
    keys,
    values,
    mixed,
    tops,
    sums,
    heads,
    o_part,
    o_0,
    o_1,
    o_2,
    o_3,
    o_4,
    result,
    gain,
    tile_count,
    text_start,
    result_sem,
    local_sem,
    stage_sem,
    sends,
    recvs,
):
    dp, mp = lax.axis_index("dp"), lax.axis_index("mp")
    core, spot = lax.rem(mp, CORES), lax.div(mp, CORES)
    low, high = lax.rem(spot, 2), lax.div(spot, 2)
    spot_1 = spot + 1 - 2 * low
    spot_2 = spot + 2 - 4 * high
    spot_3 = spot_1 + 2 - 4 * high
    dp_x = dp + 1 - 2 * lax.rem(dp, 2)
    dp_y = dp + 2 - 4 * lax.div(dp, 2)
    pc = {"mp": spot * CORES + 1 - core}
    x1, y1 = {"dp": dp_x}, {"dp": dp_y}
    z1 = {"mp": spot_1 * CORES + core}
    z2 = {"mp": spot_2 * CORES + core}

    barrier = pltpu.get_barrier_semaphore()
    for peer in (pc, x1, y1, z1, z2):
        pl.semaphore_signal(barrier, inc=1, device_id=peer, device_id_type=MESH)

    locals_ = []

    def local(source, target):
        copy = pltpu.make_async_copy(source, target, local_sem.at[len(locals_)])
        copy.start()
        locals_.append(copy)
        return copy

    rows = image.shape[0]
    hidden = fc1.shape[0]
    part_rows = rows_part.shape[0]
    depth = staged.shape[1]
    stages = staged.shape[0]

    def q_copy(step):
        slot = lax.rem(step, stages)
        return pltpu.make_async_copy(
            q_weight.at[pl.ds(pl.multiple_of(step * depth, depth), depth)],
            staged.at[slot],
            stage_sem.at[slot],
        )

    def o_copy(step):
        slot = lax.rem(step, stages)
        return pltpu.make_async_copy(
            o_weight.at[:, pl.ds(pl.multiple_of(step * depth, depth), depth)],
            staged.at[slot],
            stage_sem.at[slot],
        )

    small_copies = [
        local(gain_from, gain),
        local(tiles_from, tile_count),
        local(start_from, text_start),
    ]
    image_copy = local(image, pixels.at[0])
    up_copy = local(fc1, up.at[0, pl.ds(0, hidden)])
    down_copy = local(fc2, down.at[0, pl.ds(0, hidden)])
    text_copy = local(text, words)
    for step in range(stages):
        q_copy(step).start()
    kv_copy = local(kv, kv_raw)
    part_copy = local(
        projector.at[pl.ds(pl.multiple_of(dp * part_rows, part_rows), part_rows)], rows_part
    )

    pl.semaphore_wait(barrier, 5)

    started = []

    def remote(source, target, peer):
        slot = len(started)
        copy = pltpu.make_async_remote_copy(
            src_ref=source,
            dst_ref=target,
            send_sem=sends.at[slot],
            recv_sem=recvs.at[slot],
            device_id=peer,
            device_id_type=MESH,
        )
        copy.start()
        started.append(copy)
        return copy

    mine, theirs = pl.ds(0, hidden), pl.ds(hidden, hidden)
    parts = x_send.shape[1]
    slim = rows // parts
    slices = [pl.ds(part * slim, slim) for part in range(parts)]
    quarter = rows // 4
    quarters = [pl.ds(begin, quarter) for begin in range(0, rows, quarter)]
    piece = 32
    bits = [pl.ds(begin, piece) for begin in range(0, hidden, piece)]
    image_z, up_z, down_z = [], [], []
    pieces = [(fc1, up, up_z, area) for area in bits]
    pieces += [(fc2, down, down_z, area) for area in bits]

    def image_out():
        area = quarters[len(image_z)]
        image_z.append(remote(image.at[area], pixels.at[2, area], z1))

    for number, (source, target, group, area) in enumerate(pieces):
        if number % 2 == 0 and len(image_z) < len(quarters):
            image_out()
        group.append(remote(source.at[area], target.at[2, area], z2))
    while len(image_z) < len(quarters):
        image_out()
    image_x = remote(image, pixels.at[1], x1)
    up_y = remote(fc1, up.at[1, mine], y1)
    down_y = remote(fc2, down.at[1, mine], y1)
    up_p = {0: remote(fc1, up.at[0, theirs], pc)}
    down_p = {0: remote(fc2, down.at[0, theirs], pc)}

    text_copy.wait()
    q_steps = q_weight.shape[0] // depth
    q_total[...] = jnp.zeros_like(q_total)

    def q_step(step, carry):
        q_copy(step).wait()
        q_total[...] += jnp.dot(
            words[:, pl.ds(pl.multiple_of(step * depth, depth), depth)],
            staged[lax.rem(step, stages)],
            preferred_element_type=jnp.float32,
        )

        @pl.when(step + stages < q_steps)
        def _():
            q_copy(step + stages).start()

        return carry

    lax.fori_loop(0, q_steps, q_step, 0)
    text_rows = words.shape[0]
    head_count = q_total.shape[1] // HEAD_DIM
    for head in range(head_count):
        queries[head // 2, pl.ds(head % 2 * text_rows, text_rows)] = q_total[
            :, head * HEAD_DIM : (head + 1) * HEAD_DIM
        ].astype(jnp.bfloat16)

    strip = 32

    def normalise(block):
        def one(step, carry):
            spot_rows = pl.ds(pl.multiple_of(step * strip, strip), strip)
            entry = pixels[block, spot_rows].astype(jnp.float32)
            normed[block, spot_rows] = layer_norm(entry, gain[...]).astype(jnp.bfloat16)
            return carry

        lax.fori_loop(0, rows // strip, one, 0)

    tile = 256

    def mlp(block, first, last, base, stride=1):
        def one(step, carry):
            row = base + step * stride
            inner = lax.dot_general(
                normed[row], up[block], (((1,), (1,)), ((), ())), preferred_element_type=jnp.float32
            )
            inner = erf_gelu(inner).astype(jnp.bfloat16)
            for begin in range(0, total.shape[-1], tile):
                area = pl.ds(begin, tile)
                term = jnp.dot(inner, down[block, :, area], preferred_element_type=jnp.float32)
                if first:
                    total[row, :, area] = term
                else:
                    total[row, :, area] += term
            return carry

        lax.fori_loop(0, last, one, 0)

    def widen(block, last, base, stride=1):
        def one(step, carry):
            row = base + step * stride
            inner = lax.dot_general(
                normed[row], up[block], (((1,), (1,)), ((), ())), preferred_element_type=jnp.float32
            )
            held[block - 2, row] = erf_gelu(inner).astype(jnp.bfloat16)
            return carry

        lax.fori_loop(0, last, one, 0)

    def narrow(block, last, base, stride=1):
        def one(step, carry):
            row = base + step * stride
            for begin in range(0, total.shape[-1], tile):
                area = pl.ds(begin, tile)
                total[row, :, area] += jnp.dot(
                    held[block - 2, row], down[block, :, area], preferred_element_type=jnp.float32
                )
            return carry

        lax.fori_loop(0, last, one, 0)

    for copy in small_copies:
        copy.wait()
    image_copy.wait()
    up_copy.wait()
    down_copy.wait()
    normalise(0)
    up_p[0].wait_recv()
    down_p[0].wait_recv()
    mlp(0, True, 1, 0)
    kv_copy.wait()
    flat = 16

    def flatten(step, carry):
        area = pl.ds(pl.multiple_of(step * flat, flat), flat)
        kv_flat[area] = kv_raw[area].reshape(flat, kv_flat.shape[1])
        return carry

    lax.fori_loop(0, kv_flat.shape[0] // flat, flatten, 0)
    part_copy.wait()
    columns = fold_part.shape[-1]

    def fold_step(head, carry):
        block = kv_flat[:, pl.ds(pl.multiple_of(head * columns, columns), columns)]
        fold_part[lax.div(head, CORES), lax.rem(head, CORES)] = jnp.dot(
            rows_part[...], block, preferred_element_type=jnp.float32
        ).astype(jnp.bfloat16)
        return carry

    lax.fori_loop(0, fold_part.shape[0] * CORES, fold_step, 0)
    fold_p = remote(fold_part.at[:, 1 - core], fold_0, pc)
    for step in range(stages):
        o_copy(step).start()
    image_x.wait_recv()
    normalise(1)
    mlp(0, True, 1, 1)
    up_y.wait_recv()
    up_p[1] = remote(up.at[1, mine], up.at[1, theirs], pc)
    down_y.wait_recv()
    down_p[1] = remote(down.at[1, mine], down.at[1, theirs], pc)
    up_d, down_d = [], []
    for part, copy in enumerate(up_z):
        copy.wait_recv()
        up_d.append(remote(up.at[2, bits[part]], up.at[3, bits[part]], y1))
    up_p[2] = remote(up.at[2, mine], up.at[2, theirs], pc)
    image_d, shared = [], []

    def image_on(part):
        image_z[part].wait_recv()
        image_d.append(remote(pixels.at[2, quarters[part]], pixels.at[3, quarters[part]], x1))

    def down_on(part):
        down_z[part].wait_recv()
        down_d.append(remote(down.at[2, bits[part]], down.at[3, bits[part]], y1))
        mirror = pl.ds(hidden + part * piece, piece)
        shared.append(remote(down.at[2, bits[part]], down.at[2, mirror], pc))

    image_on(0)
    image_on(1)
    up_p[1].wait_recv()
    down_p[1].wait_recv()
    mlp(1, False, 2, 0)
    image_on(2)
    up_p[2].wait_recv()
    widen(2, 2, 0)
    down_on(0)
    image_on(3)
    down_on(1)
    normalise(2)
    mlp(0, True, 1, 2)
    mlp(1, False, 1, 2)
    for copy in up_d:
        copy.wait_recv()
    up_p[3] = remote(up.at[3, mine], up.at[3, theirs], pc)
    for part in range(2, len(bits)):
        down_on(part)
    fold_p.wait_recv()
    spots = fold_0.shape[0]

    def fold_pair(index, carry):
        fold_1[lax.div(index, 2), lax.rem(index, 2)] = (
            fold_part[index, core].astype(jnp.float32) + fold_0[index].astype(jnp.float32)
        ).astype(jnp.bfloat16)
        return carry

    lax.fori_loop(0, spots, fold_pair, 0)
    fold_z = remote(fold_1.at[:, 1 - low], fold_2, z1)
    up_p[3].wait_recv()
    widen(3, 1, 1)
    for copy in image_d:
        copy.wait_recv()
    normalise(3)
    spread = []

    def relay(part):
        down_d[part].wait_recv()
        mirror = pl.ds(hidden + part * piece, piece)
        spread.append(remote(down.at[3, bits[part]], down.at[3, mirror], pc))

    for part in range(2):
        relay(part)
    mlp(0, True, 1, 3)
    mlp(1, False, 1, 3)
    for part in range(2, len(bits)):
        relay(part)
    for copy in shared:
        copy.wait_recv()
    widen(2, 1, 3)
    narrow(2, 1, 3)
    widen(3, 1, 3)
    for copy in spread:
        copy.wait_recv()

    def to_x(row, part):
        index = row // 2
        x_send[index, part] = total[row, slices[part]].astype(jnp.bfloat16)
        return remote(x_send.at[index, part], x_recv.at[index, part], x1)

    narrow(3, 1, 3)
    x_copies = {(1, part): to_x(3, part) for part in range(parts)}
    narrow(2, 1, 1)
    narrow(3, 1, 1)
    for part in range(parts):
        x_copies[0, part] = to_x(1, part)
    widen(2, 1, 2)
    widen(3, 1, 2)
    narrow(2, 1, 2)
    narrow(3, 1, 2)
    widen(3, 1, 0)
    narrow(2, 1, 0)
    narrow(3, 1, 0)
    fold_z.wait_recv()
    for index in range(2):
        fold_3[index] = (
            fold_1[index, low].astype(jnp.float32) + fold_2[index].astype(jnp.float32)
        ).astype(jnp.bfloat16)
    fold_zz = remote(fold_3.at[1 - high], fold_4, z2)

    def fold_rows(owner):
        return folded.at[pl.ds(pl.multiple_of(owner * part_rows, part_rows), part_rows)]

    z_copies, pairs, onward = {}, {}, {}

    def area_of(core_side, part):
        group, inside = part // (parts // 2), part % (parts // 2)
        return pl.ds(group * rows + core_side * (rows // 2) + inside * slim, slim)

    def to_partner(unit, part):
        pairs[unit, part] = remote(
            encoded.at[unit, area_of(0, part)], encoded.at[unit, area_of(1, part)], pc
        )

    for part in range(parts):
        x_copies[1, part].wait_recv()
        z_send[part] = (
            total[2, slices[part]] + x_recv[1, part].astype(jnp.float32)
        ).astype(jnp.bfloat16)
        z_copies[part] = remote(z_send.at[part], z_recv.at[part], z1)
        if part == 1:
            fold_zz.wait_recv()
            fold_own[...] = (
                fold_3[high].astype(jnp.float32) + fold_4[...].astype(jnp.float32)
            ).astype(jnp.bfloat16)
            fold_local = local(fold_own, fold_rows(dp))
            fold_y = remote(fold_own, fold_rows(dp), y1)
            fold_x = remote(fold_own, fold_rows(dp), x1)
    for part in range(parts):
        x_copies[0, part].wait_recv()
        z_copies[part].wait_recv()
        area = slices[part]
        encoded[0, area_of(0, part)] = (
            pixels[0, area].astype(jnp.float32)
            + total[0, area]
            + x_recv[0, part].astype(jnp.float32)
            + z_recv[part].astype(jnp.float32)
        ).astype(jnp.bfloat16)
        for unit, peer in ((2, z2), (1, z1)):
            onward[unit, part] = remote(
                encoded.at[0, area_of(0, part)], encoded.at[unit, area_of(0, part)], peer
            )
        to_partner(0, part)
    fold_x.wait_recv()
    fold_d = remote(fold_rows(dp_x), fold_rows(dp_x), y1)

    def pass_on(part):
        onward[1, part].wait_recv()
        to_partner(1, part)
        onward[2, part].wait_recv()
        onward[3, part] = remote(
            encoded.at[2, area_of(0, part)], encoded.at[3, area_of(0, part)], z1
        )
        to_partner(2, part)

    def gather(unit, begin=0, end=parts):
        for part in range(begin, end):
            pairs[unit, part].wait_recv()

    for part in range(parts // 2):
        pass_on(part)
    fold_local.wait()
    fold_y.wait_recv()
    fold_d.wait_recv()
    scale = 1.0 / HEAD_DIM**0.5
    limit = tile_count[0] * TILE_TOK

    def attend(unit, unit_spot, begin=0, count=2 * rows):
        area = pl.ds(0, count)
        kv_block = jnp.dot(
            encoded[unit, pl.ds(begin, count)], folded[...], preferred_element_type=jnp.float32
        )
        key = kv_block[:, :HEAD_DIM]
        key_scale = lax.rsqrt(jnp.mean(key * key, axis=-1, keepdims=True) + 1e-06)
        keys[area] = (key * key_scale).astype(jnp.bfloat16)
        values[area] = kv_block[:, HEAD_DIM:].astype(jnp.bfloat16)
        place = begin + lax.broadcasted_iota(jnp.int32, (1, count), 1)
        group = jnp.where(place < rows, 0, 1)
        inside = place - group * rows
        mine_here = inside < rows // 2
        own_base = (unit_spot * CORES + core) * rows
        other_base = (unit_spot * CORES + 1 - core) * rows - rows // 2
        token = inside + group * (rows // 2) + jnp.where(mine_here, own_base, other_base)
        valid = token < limit

        def one(index, carry):
            scores = (
                lax.dot_general(
                    queries[index],
                    keys[area],
                    (((1,), (1,)), ((), ())),
                    preferred_element_type=jnp.float32,
                )
                * scale
            )
            scores = jnp.where(valid, scores, -1e30)
            top = jnp.max(scores, axis=-1, keepdims=True)
            if unit > 0:
                before = tops[index][:, :1]
                top = jnp.maximum(before, top)
                shrink = jnp.exp(before - top)
            weights = jnp.exp(scores - top)
            weight_sum = jnp.sum(weights, axis=-1, keepdims=True)
            blend = jnp.dot(
                weights.astype(jnp.bfloat16), values[area], preferred_element_type=jnp.float32
            )
            if unit > 0:
                weight_sum += shrink * sums[index][:, :1]
                blend += shrink * mixed[index]
            tops[index] = jnp.broadcast_to(top, tops.shape[1:])
            sums[index] = jnp.broadcast_to(weight_sum, sums.shape[1:])
            mixed[index] = blend
            return carry

        lax.fori_loop(0, queries.shape[0], one, 0)

    gather(0)
    attend(0, spot)
    for part in range(parts // 2, parts):
        pass_on(part)
    gather(1)
    attend(1, spot_1)
    gather(2)
    attend(2, spot_2)
    for part in range(parts):
        onward[3, part].wait_recv()
        to_partner(3, part)
    gather(3)
    attend(3, spot_3)

    text_at = lax.broadcasted_iota(jnp.int32, (text_rows, 1), 0)
    row_mask = (text_at >= text_start[0]).astype(jnp.float32)
    for head in range(head_count):
        area = pl.ds(head % 2 * text_rows, text_rows)
        heads[:, head * HEAD_DIM : (head + 1) * HEAD_DIM] = (
            mixed[head // 2, area] / sums[head // 2, area][:, :1] * row_mask
        ).astype(jnp.bfloat16)

    steps = o_part.shape[0]
    base = len(started)

    def o_remote(kind, step, source, target, peer):
        return pltpu.make_async_remote_copy(
            src_ref=source,
            dst_ref=target,
            send_sem=sends.at[base + kind * steps + step],
            recv_sem=recvs.at[base + kind * steps + step],
            device_id=peer,
            device_id_type=MESH,
        )

    def o_first(step):
        return o_remote(0, step, o_part.at[step, :, :, 1 - core], o_0.at[step], pc)

    def o_second(step):
        return o_remote(1, step, o_1.at[step, :, 1 - low], o_2.at[step], z1)

    def o_third(step):
        return o_remote(2, step, o_3.at[step, 1 - high], o_4.at[step], z2)

    def meet_first(step):
        o_first(step).wait_recv()
        o_1[step] = (
            o_part[step, :, :, core].astype(jnp.float32) + o_0[step].astype(jnp.float32)
        ).astype(jnp.bfloat16)
        o_second(step).start()

    def meet_second(step):
        o_second(step).wait_recv()
        o_3[step] = (
            o_1[step, :, low].astype(jnp.float32) + o_2[step].astype(jnp.float32)
        ).astype(jnp.bfloat16)
        o_third(step).start()

    def o_step(step, carry):
        o_copy(step).wait()
        slot = lax.rem(step, stages)
        result = jnp.dot(heads[...], staged[slot], preferred_element_type=jnp.float32)
        o_part[step] = result.reshape(o_part.shape[1:]).astype(jnp.bfloat16)
        o_first(step).start()

        @pl.when(step + stages < steps)
        def _():
            o_copy(step + stages).start()

        @pl.when(step > 1)
        def _():
            meet_first(step - 2)

        return carry

    lax.fori_loop(0, steps, o_step, 0)
    meet_first(steps - 2)
    meet_first(steps - 1)

    def second(step, carry):
        meet_second(step)
        return carry

    lax.fori_loop(0, steps, second, 0)

    def result_copy(step):
        return pltpu.make_async_copy(
            result.at[step],
            out.at[:, pl.ds(pl.multiple_of(step * depth, depth), depth)],
            result_sem.at[step],
        )

    def third(step, carry):
        o_third(step).wait_recv()
        result[step] = (
            o_3[step, high].astype(jnp.float32) + o_4[step].astype(jnp.float32)
        ).astype(jnp.bfloat16)
        result_copy(step).start()
        return carry

    lax.fori_loop(0, steps, third, 0)
    for copy in started:
        copy.wait_send()

    def drain(step, carry):
        o_first(step).wait_send()
        o_second(step).wait_send()
        o_third(step).wait_send()
        result_copy(step).wait()
        return carry

    lax.fori_loop(0, steps, drain, 0)


def fused(image, gain, fc1, fc2, projector, kv, text, q_weight, o_weight, tile_count, text_start):
    rows, width = image.shape
    hidden = fc1.shape[0]
    part_rows = projector.shape[0] // lax.axis_size("dp")
    depth = projector.shape[1]
    kv_columns = kv.shape[1] * kv.shape[2] * kv.shape[3]
    columns = kv_columns // lax.axis_size("mp")
    text_rows = text.shape[0]
    query_columns = q_weight.shape[1]
    pairs = query_columns // HEAD_DIM // 2
    parts = 4
    token_rows = text_rows // lax.axis_size("mp")
    steps = o_weight.shape[1] // depth
    low, wide = jnp.bfloat16, jnp.float32
    copies = 144 + 3 * steps
    scratch = [
        ((4, 2 * hidden, width), low),
        ((4, 2 * hidden, width), low),
        ((4, rows, width), low),
        ((4, rows, width), low),
        ((4, rows, width), wide),
        ((2, 4, rows, 2 * hidden), low),
        ((2, parts, rows // parts, width), low),
        ((2, parts, rows // parts, width), low),
        ((parts, rows // parts, width), low),
        ((parts, rows // parts, width), low),
        ((4, 2 * rows, width), low),
        ((part_rows, depth), low),
        (kv.shape, low),
        ((kv.shape[0], kv_columns), low),
        ((4, CORES, part_rows, columns), low),
        ((4, part_rows, columns), low),
        ((2, 2, part_rows, columns), low),
        ((2, part_rows, columns), low),
        ((2, part_rows, columns), low),
        ((part_rows, columns), low),
        ((part_rows, columns), low),
        ((width, columns), low),
        (text.shape, low),
        ((4, depth, depth), low),
        ((text_rows, query_columns), wide),
        ((pairs, 2 * text_rows, HEAD_DIM), low),
        ((2 * rows, HEAD_DIM), low),
        ((2 * rows, HEAD_DIM), low),
        ((pairs, 2 * text_rows, HEAD_DIM), wide),
        ((pairs, 2 * text_rows, HEAD_DIM), wide),
        ((pairs, 2 * text_rows, HEAD_DIM), wide),
        ((text_rows, query_columns), low),
        ((steps, 2, 2, CORES, token_rows, depth), low),
        ((steps, 2, 2, token_rows, depth), low),
        ((steps, 2, 2, token_rows, depth), low),
        ((steps, 2, token_rows, depth), low),
        ((steps, 2, token_rows, depth), low),
        ((steps, token_rows, depth), low),
        ((steps, token_rows, depth), low),
        (gain.shape, wide),
    ]
    anywhere = pl.BlockSpec(memory_space=pl.ANY)
    return pl.pallas_call(
        fused_kernel,
        out_shape=jax.ShapeDtypeStruct((token_rows, o_weight.shape[1]), jnp.bfloat16),
        in_specs=[anywhere] * 11,
        out_specs=anywhere,
        scratch_shapes=[pltpu.VMEM(shape, kind) for shape, kind in scratch]
        + [
            pltpu.SMEM(tile_count.shape, jnp.int32),
            pltpu.SMEM(text_start.shape, jnp.int32),
            pltpu.SemaphoreType.DMA((steps,)),
            pltpu.SemaphoreType.DMA((16,)),
            pltpu.SemaphoreType.DMA((4,)),
            pltpu.SemaphoreType.DMA((copies,)),
            pltpu.SemaphoreType.DMA((copies,)),
        ],
        compiler_params=pltpu.CompilerParams(
            collective_id=7, has_side_effects=True, vmem_limit_bytes=67043328
        ),
        name="fused",
    )(image, gain, fc1, fc2, projector, kv, text, q_weight, o_weight, tile_count, text_start)


def paired_local(
    image,
    ln_gain,
    fc1_weight,
    fc2_weight,
    projector_weight,
    kv_weight,
    text,
    q_weight,
    o_weight,
    tile_count,
    text_start,
):
    return fused(
        image[0],
        ln_gain,
        fc1_weight.T,
        fc2_weight,
        projector_weight,
        kv_weight,
        text[0],
        q_weight,
        o_weight,
        tile_count,
        text_start,
    )[None]


def choose(*arrays):
    groups, members = lax.axis_size("dp"), lax.axis_size("mp")
    pairs_of_pairs = groups == members // CORES == 2 * 2
    if pairs_of_pairs and arrays[5].shape[1] == members:
        return paired_local(*arrays)
    return local(*arrays)


def solution(mesh):
    return jax.shard_map(
        choose,
        mesh=mesh,
        in_specs=(
            P("dp", "mp", None),
            P(),
            P(None, ("dp", "mp")),
            P(("dp", "mp"), None),
            P(None, "mp"),
            P("mp", None, None, None),
            P("dp", None, None),
            P(None, "mp"),
            P("mp", None),
            P("dp"),
            P("dp"),
        ),
        out_specs=P("dp", "mp", None),
        check_vma=False,
    )
```
